32 devices in a mesh: row: 8 (over y, x, core), col: 4 (over z).
Axes of the slice: x: 2, y: 2, z: 4, core: 2. Of those that a mesh axis runs over, the one named last changes fastest.
Arguments:
- stiff_bb: bfloat16 [96, 3, 128, 384], P(('row', 'col')), may hold values from -6 to 6
- stiff_bi: bfloat16 [96, 384, 3072], P(('row', 'col')), may hold values from -6 to 6
- constraint_modes: bfloat16 [96, 3072, 384], P(('row', 'col')), may hold values from -0.109375 to 0.109375
- interior_mass: float32 [96, 3072], P(('row', 'col')), may hold values from 0.25 to 4
- fixed_modes: bfloat16 [96, 3072, 256], P(('row', 'col')), may hold values from -6 to 6
- mass_bb: bfloat16 [96, 3, 128, 384], P(('row', 'col')), may hold values from -6 to 6
- boundary_map: int32 [96, 3], P(('row', 'col')), may hold values from 0 to 191, as said below
Outputs:
- interface_stiffness: float32 [192, 4, 128, 128], P('row', None, 'col')
- interface_mass: float32 [192, 4, 128, 128], P('row', None, 'col')
- mass_coupling: float32 [96, 256, 384], P(('row', 'col'))
The draws below stay inside these ranges and needn't reach their ends.
Inputs may be any that keep to these rules, and one draw needn't show every extreme that they name: `boundary_map`: row s holds blocks b, b + a, b + c with 0 < a < c < 4, all three in the range of one owner (block // 24). Rows come in aligned row groups of 12; no owner serves more than 2 rows of one row group, and in every draw one owner serves exactly 2 rows of every row group.
All inputs are finite; a program needn't handle non-finite values.
Results may differ from the reference program's by a relative error of at most 0.0029.
Values sent between devices are 32-bit elements; how exact they have to be, the bound alone decides.
A program may use at most 192 MiB of HBM per device.

```python
import math
import jax
import jax.numpy as jnp
from jax import lax

NI = 3072
BLK = 128
NB = 384
NM = 256
BAND = 4
BPO = 24
SE_GRP = 12
CAP = 2
SETOT = 96
NBLOCK = 192
N_ROW = 8


def draw_boundary_map(key, part):
    slot_count = N_ROW * CAP
    keys = jax.random.split(jax.random.fold_in(key, 17), 7)
    priority_tiers = jax.random.randint(keys[0], (N_ROW,), 0, 4)
    busiest_targets = jax.random.randint(keys[1], (), 0, N_ROW)
    position_owner = jnp.arange(slot_count) // CAP
    random_jitter = jax.random.randint(keys[2], (N_ROW, slot_count), 0, 65536)
    extra_credit = jnp.where(position_owner == busiest_targets, 1 << 20, 0)
    ranking_values = random_jitter + priority_tiers[position_owner][None, :] * 16384 + extra_credit[None, :]
    ranking_values = ranking_values * slot_count + jnp.arange(slot_count)[None, :]
    picked = lax.top_k(ranking_values, SE_GRP)[1]
    order_scores = jax.random.randint(keys[3], (N_ROW, SE_GRP), 0, 4096) * SE_GRP + jnp.arange(SE_GRP)[None, :]
    order = lax.top_k(order_scores, SE_GRP)[1]
    picked = jnp.take_along_axis(picked, order, axis=1)
    owners = (picked // CAP).reshape(SETOT)
    first = jax.random.randint(keys[4], (SETOT,), 1, BAND - 1)
    second = first + jax.random.randint(keys[5], (SETOT,), 1, BAND - first)
    start = owners * BPO + jax.random.randint(keys[6], (SETOT,), 0, BPO - second)
    return jnp.stack([start, start + first, start + second], axis=1).astype(jnp.int32)


def steps_of(rng, extent, cuts, low, top_value):
    gain, own = 1.0, jax.random.fold_in(rng, 6)
    for position, blocks in cuts:
        steps = jnp.exp(jax.random.uniform(jax.random.fold_in(own, position), (blocks,), jnp.float32, low / len(cuts), top_value / len(cuts)))
        gain = gain * jnp.repeat(steps, extent[position] // blocks).reshape([-1 if axis == position else 1 for axis in range(len(extent))])
    return gain


def centred(key, extent, deviation, most, pieces=(), dtype=jnp.bfloat16):
    array = deviation * jax.random.normal(key, extent, jnp.float32)
    if pieces:
        array = array * steps_of(key, extent, pieces, -0.22, 0.18)
    return jnp.clip(array, -most, most).astype(dtype)


def setup_inputs(seed: int = 0) -> dict:
    streams_of = jax.random.split(jax.random.key(seed), 8)
    return {
        "stiff_bb": centred(streams_of[0], (SETOT, 3, BLK, NB), 1.0, 6.0, ((0, 32),)),
        "stiff_bi": centred(streams_of[1], (SETOT, NB, NI), 1.0, 6.0, ((0, 32),)),
        "constraint_modes": centred(streams_of[2], (SETOT, NI, NB), NI ** -0.5, 0.109375, ((0, 32),)),
        "interior_mass": jnp.clip(jnp.exp(math.log(4.0) - 2.7725887 * jax.random.uniform(streams_of[3], (SETOT, NI), jnp.float32) ** steps_of(streams_of[3], (SETOT, NI), ((0, 32),), -0.2, 0.2)), 0.25, 4.0),
        "fixed_modes": centred(streams_of[4], (SETOT, NI, NM), 1.0, 6.0, ((0, 32),)),
        "mass_bb": centred(streams_of[5], (SETOT, 3, BLK, NB), 1.0, 6.0, ((0, 32),)),
        "boundary_map": draw_boundary_map(jax.random.fold_in(streams_of[7], 71), 0),
    }


PAIRS = ((0, 0), (1, 1), (2, 2), (0, 1), (0, 2), (1, 2))


def reduce_one(items):
    block_bb, block_bi, psi, masses, modes, mass_block = items
    order = block_bi.shape[0]
    weighted = (masses[:, None] * psi.astype(jnp.float32)).astype(jnp.bfloat16)
    red_k = block_bb.reshape(order, order).astype(jnp.float32) + jnp.dot(block_bi, psi, preferred_element_type=jnp.float32)
    red_m = mass_block.reshape(order, order).astype(jnp.float32) + jnp.dot(psi.T, weighted, preferred_element_type=jnp.float32)
    coupling = jnp.dot(modes.T, weighted, preferred_element_type=jnp.float32)
    return red_k, red_m, coupling


def reference(stiff_bb, stiff_bi, constraint_modes, interior_mass, fixed_modes, mass_bb, boundary_map):
    red_k, red_m, coupling = lax.map(reduce_one, (stiff_bb, stiff_bi, constraint_modes, interior_mass, fixed_modes, mass_bb))
    width = stiff_bb.shape[2]
    total_k = jnp.zeros((NBLOCK, BAND, width, width), jnp.float32)
    total_m = jnp.zeros((NBLOCK, BAND, width, width), jnp.float32)
    for first, second in PAIRS:
        rows = boundary_map[:, first].astype(jnp.int32)
        offset = (boundary_map[:, second] - boundary_map[:, first]).astype(jnp.int32)
        piece_k = red_k[:, first * width:(first + 1) * width, second * width:(second + 1) * width]
        piece_m = red_m[:, first * width:(first + 1) * width, second * width:(second + 1) * width]
        total_k = total_k.at[rows, offset].add(piece_k)
        total_m = total_m.at[rows, offset].add(piece_m)
    return total_k, total_m, coupling
```

```python
import functools
import jax
import jax.numpy as jnp
from jax import lax
from jax.experimental import pallas as pl
from jax.experimental.pallas import tpu as pltpu
from jax.sharding import PartitionSpec as P

BAND = 4
BPO = 24
LANE = 128

PAIRS = ((0, 0), (0, 1), (1, 1), (1, 2), (2, 2), (0, 2))
KINDS = 2
CHUNKS = KINDS * len(PAIRS)
AHEAD = 2
PIECES = 4
MESH = pl.DeviceIdType.MESH
VMEM_LIMIT = 60 * 1024 * 1024


def at_col(z):
    return {"row": lax.axis_index("row"), "col": z}


def at_row(r):
    return {"row": r, "col": lax.axis_index("col")}


def reduce_and_send(
    owners, lanes, slots,
    kbb, kbi, psi, mass, modes, mbb, table,
    got, targets, coupling,
    kbb_v, kbi_v, psi_v, modes_v, mbb_v, weighted, coupled,
    reduced, grouped, staging, outgoing, table_v, maps_v, all_v, maps_s, all_s,
    in_sems, z_send, z_recv, r_send, r_recv, r_own,
    zm_send, zm_recv, rm_send, rm_recv, small, out_sems, block_sems, piece_sems,
):
    count, order, inner = kbi.shape
    width = order // 3
    part = width // lanes
    members = count * lanes
    row = lax.axis_index("row")
    col = lax.axis_index("col")

    def block_load(i):
        span = pl.ds(i * width, width)
        return pltpu.make_async_copy(kbi.at[0, span], kbi_v.at[0, span], block_sems.at[i])

    def piece_load(k):
        span = pl.ds(k * (inner // PIECES), inner // PIECES)
        return pltpu.make_async_copy(psi.at[0, span], psi_v.at[0, span], piece_sems.at[k])

    def kbb_load(s):
        return pltpu.make_async_copy(kbb.at[s], kbb_v.at[s], in_sems.at[2, s])

    def loads(s):
        return (
            pltpu.make_async_copy(kbi.at[s], kbi_v.at[s], in_sems.at[0, s]),
            pltpu.make_async_copy(psi.at[s], psi_v.at[s], in_sems.at[1, s]),
            kbb_load(s),
        )

    def late_loads(s):
        return (
            pltpu.make_async_copy(mbb.at[s], mbb_v.at[s], in_sems.at[3, s]),
            pltpu.make_async_copy(modes.at[s], modes_v.at[s], in_sems.at[4, s]),
        )

    block_load(0).start()
    for k in range(PIECES):
        piece_load(k).start()
    kbb_load(0).start()
    for i in range(1, 3):
        block_load(i).start()

    barrier = pltpu.get_barrier_semaphore()
    for i in range(1, lanes):
        pl.semaphore_signal(barrier, inc=1, device_id=at_col(lax.rem(col + i, lanes)), device_id_type=MESH)

    def greet(i, carry):
        pl.semaphore_signal(barrier, inc=1, device_id=at_row(lax.rem(row + i, owners)), device_id_type=MESH)
        return carry

    lax.fori_loop(1, owners, greet, 0)

    def put(kind, s, i, strip):
        for j in range(i, 3):
            block = strip[:, (j - i) * width : (j - i + 1) * width]
            reduced[kind * len(PAIRS) + PAIRS.index((i, j)), :, s] = block.reshape(lanes, part, width)

    def stiff(s, i):
        strip = jnp.dot(
            kbi_v[s, i * width : (i + 1) * width, :], psi_v[s, :, i * width :],
            preferred_element_type=jnp.float32,
        )
        put(0, s, i, strip + kbb_v[s, i, :, i * width :].astype(jnp.float32))

    def z_map(i):
        return pltpu.make_async_remote_copy(
            src_ref=table_v, dst_ref=maps_v.at[col],
            send_sem=zm_send.at[i], recv_sem=zm_recv.at[lanes - i],
            device_id=at_col(lax.rem(col + i, lanes)), device_id_type=MESH,
        )

    def z_copy(p, i):
        to = lax.rem(col + i, lanes)
        return pltpu.make_async_remote_copy(
            src_ref=reduced.at[p, to], dst_ref=grouped.at[p, col],
            send_sem=z_send.at[p, i], recv_sem=z_recv.at[p, lanes - i],
            device_id=at_col(to), device_id_type=MESH,
        )

    def z_copy_part(p, first, size, i):
        to = lax.rem(col + i, lanes)
        return pltpu.make_async_remote_copy(
            src_ref=reduced.at[p, to, pl.ds(first, size)], dst_ref=grouped.at[p, col, pl.ds(first, size)],
            send_sem=z_send.at[p, i], recv_sem=z_recv.at[p, lanes - i],
            device_id=at_col(to), device_id_type=MESH,
        )

    def r_map(i):
        return pltpu.make_async_remote_copy(
            src_ref=maps_v, dst_ref=all_v.at[row],
            send_sem=rm_send.at[i], recv_sem=rm_recv.at[owners - i],
            device_id=at_row(lax.rem(row + i, owners)), device_id_type=MESH,
        )

    half = len(PAIRS)
    place = (lax.broadcasted_iota(jnp.int32, (8, LANE), 0), lax.broadcasted_iota(jnp.int32, (8, LANE), 1))
    tile = jnp.zeros((8, LANE), jnp.int32)
    for s in range(count):
        for k in range(3):
            tile = jnp.where((place[0] == 0) & (place[1] == 3 * s + k), table[s, k], tile)
    table_v[...] = tile
    maps_v[col] = tile

    for k in range(PIECES):
        piece_load(k).wait()
    kbb_load(0).wait()
    for i in range(3):
        block_load(i).wait()
        if i == 0:
            for later in range(1, count):
                for copy in loads(later):
                    copy.start()
        stiff(0, i)
        if i == 0:
            pl.semaphore_wait(barrier, lanes - 1 + owners - 1)
            for k in range(1, lanes):
                z_map(k).start()
        for j in range(i, 3):
            for k in range(1, lanes):
                z_copy_part(PAIRS.index((i, j)), 0, 1, k).start()

    for s in range(count):
        for copy in late_loads(s):
            copy.start()

    def stiffs(s, carry):
        for copy in loads(s):
            copy.wait()
        for i in range(3):
            stiff(s, i)
        return carry

    lax.fori_loop(1, count, stiffs, 0)

    def send_rest(p):
        for i in range(1, lanes):
            z_copy_part(p, 1, count - 1, i).start()

    def send_chunk(p):
        for i in range(1, lanes):
            z_copy(p, i).start()

    for p in range(AHEAD):
        send_rest(p)

    def masses(s, carry):
        for copy in late_loads(s):
            copy.wait()
        pick = lax.broadcasted_iota(jnp.int32, (count, inner), 0) == s
        line = jnp.sum(jnp.where(pick, mass[...], 0.0), axis=0, keepdims=True)
        steps = inner // LANE
        lines = [line[:, k * LANE : (k + 1) * LANE] for k in range(steps)]
        filler = jnp.zeros((-steps % LANE, LANE), jnp.float32)
        columns = jnp.concatenate(lines + [filler], axis=0).T
        for k in range(steps):
            span = pl.ds(k * LANE, LANE)
            scale = jnp.broadcast_to(columns[:, k : k + 1], (LANE, order))
            weighted[s, span, :] = (scale * psi_v[s, span, :].astype(jnp.float32)).astype(jnp.bfloat16)
        for i in range(3):
            strip = lax.dot_general(
                psi_v[s, :, i * width : (i + 1) * width], weighted[s, :, i * width :], across,
                preferred_element_type=jnp.float32,
            )
            put(1, s, i, strip + mbb_v[s, i, :, i * width :].astype(jnp.float32))
        return carry

    across = (((0,), (0,)), ((), ()))
    lax.fori_loop(0, count, masses, 0)

    for i in range(1, lanes):
        z_map(i).wait()
    to_scalar = pltpu.make_async_copy(maps_v, maps_s, small.at[0])
    to_scalar.start()
    lax.fori_loop(1, owners, lambda i, c: (r_map(i).start(), c)[1], 0)
    all_v[row] = maps_v[...]

    def couple(s, carry):
        coupled[s] = lax.dot_general(modes_v[s], weighted[s], across, preferred_element_type=jnp.float32)
        pltpu.make_async_copy(coupled.at[s], coupling.at[s], out_sems.at[s]).start()
        return carry


    def keep(p, carry):
        grouped[p, col] = reduced[p, col]
        return carry

    lax.fori_loop(0, CHUNKS, keep, 0)
    lax.fori_loop(0, count, couple, 0)

    to_scalar.wait()

    belongs = [maps_s[m // count, 0, 3 * (m % count)] // BPO for m in range(members)]
    ranks = []
    for m in range(members):
        rank = jnp.int32(0)
        for e in range(m):
            rank = rank + jnp.where(belongs[e] == belongs[m], 1, 0)
        ranks.append(rank)
    places = [belongs[m] * slots + ranks[m] for m in range(members)]

    chosen = []
    for slot in range(owners * slots):
        member = jnp.int32(0)
        for m in range(1, members):
            member = jnp.where(places[m] == slot, m, member)
        chosen.append(member)

    def forward(send, p, carry):
        for i in range(1, lanes):
            z_copy(p, i).wait_recv()
        if send is not None:
            send(p + AHEAD)

        staging[...] = grouped[p].reshape(members, part, width)
        for slot, member in enumerate(chosen):
            outgoing[p, slot // slots, slot % slots] = staging[member]

        def ship(i, inner_carry):
            r_copy(p, i).start()
            return inner_carry

        lax.fori_loop(1, owners, ship, 0)
        own_copy(p).start()
        return carry

    def r_copy(p, i):
        to = lax.rem(row + i, owners)
        return pltpu.make_async_remote_copy(
            src_ref=outgoing.at[p, to], dst_ref=got.at[p, row],
            send_sem=r_send.at[p], recv_sem=r_recv.at[p],
            device_id=at_row(to), device_id_type=MESH,
        )

    def own_copy(p):
        return pltpu.make_async_copy(outgoing.at[p, row], got.at[p, row], r_own.at[p])

    lax.fori_loop(1, owners, lambda i, c: (r_map(i).wait(), c)[1], 0)
    all_scalar = pltpu.make_async_copy(all_v.at[:, :, pl.ds(0, 1)], all_s, small.at[1])
    all_scalar.start()
    all_scalar.wait()

    def aim(group, carry):
        picked = [[jnp.int32(-1)] * 3 for _ in range(slots)]
        filled = jnp.int32(0)
        for m in range(members):
            at = [all_s[group, m // count, 0, 3 * (m % count) + k] for k in range(3)]
            mine = at[0] // BPO == row
            for slot in range(slots):
                hit = mine & (filled == slot)
                picked[slot] = [jnp.where(hit, at[k], picked[slot][k]) for k in range(3)]
            filled = filled + jnp.where(mine, 1, 0)
        for slot in range(slots):
            at = picked[slot]
            for p, (i, j) in enumerate(PAIRS):
                local = (at[i] - row * BPO) * BAND + at[j] - at[i]
                targets[p, group * slots + slot] = jnp.where(at[0] >= 0, local, BPO * BAND)
        return carry

    lax.fori_loop(0, owners, aim, 0)
    lax.fori_loop(0, half - AHEAD, functools.partial(forward, send_rest), 0)
    lax.fori_loop(half - AHEAD, CHUNKS - AHEAD, functools.partial(forward, send_chunk), 0)
    lax.fori_loop(CHUNKS - AHEAD, CHUNKS, functools.partial(forward, None), 0)

    def settle(p, carry):
        for i in range(1, lanes):
            z_copy(p, i).wait_send()
        rest = got.at[p, pl.ds(0, owners - 1)]
        pltpu.make_async_copy(rest, rest, r_send.at[p]).wait()
        pltpu.make_async_copy(rest, rest, r_recv.at[p]).wait()
        own_copy(p).wait()
        return carry

    lax.fori_loop(0, CHUNKS, settle, 0)
    for s in range(count):
        pltpu.make_async_copy(coupled.at[s], coupling.at[s], out_sems.at[s]).wait()


def assemble(
    owners, slots, targets, got, coupled, k_out, m_out, coupling,
    buffer, band, passing, in_sems, out_sems, pass_sems,
):
    limit = BPO * BAND

    def load(p):
        return pltpu.make_async_copy(got.at[p], buffer.at[p], in_sems.at[p])

    for p in range(CHUNKS):
        load(p).start()
    inward = pltpu.make_async_copy(coupled, passing, pass_sems.at[0])
    inward.start()
    band[...] = jnp.zeros_like(band)
    writes = []
    for kind, out in enumerate((k_out, m_out)):
        for p in range(len(PAIRS)):
            chunk = kind * len(PAIRS) + p
            load(chunk).wait()
            for place in range(owners * slots):
                at = targets[p, place]
                band[kind, at] += buffer[chunk, place // slots, place % slots]
        writes.append(pltpu.make_async_copy(band.at[kind, pl.ds(0, limit)], out, out_sems.at[kind]))
        writes[-1].start()
        if kind == 0:
            inward.wait()
            writes.append(pltpu.make_async_copy(passing, coupling, pass_sems.at[1]))
            writes[-1].start()
    for write in writes:
        write.wait()


def per_device(
    stiff_bb, stiff_bi, constraint_modes, interior_mass, fixed_modes, mass_bb, boundary_map
):
    owners = lax.axis_size("row")
    lanes = lax.axis_size("col")
    count, order, inner = stiff_bi.shape
    modes = fixed_modes.shape[2]
    width = order // 3
    part = width // lanes
    slots = (count * lanes + owners - 1) // owners
    f32, bf16 = jnp.float32, jnp.bfloat16
    hbm = pl.BlockSpec(memory_space=pl.ANY)
    vmem = pl.BlockSpec(memory_space=pltpu.VMEM)
    smem = pl.BlockSpec(memory_space=pltpu.SMEM)
    dma = pltpu.SemaphoreType.DMA
    got, targets, coupled = pl.pallas_call(
        functools.partial(reduce_and_send, owners, lanes, slots),
        out_shape=(
            jax.ShapeDtypeStruct((CHUNKS, owners, slots, part, width), f32),
            jax.ShapeDtypeStruct((len(PAIRS), owners * slots), jnp.int32),
            jax.ShapeDtypeStruct((count, modes, order), f32),
        ),
        in_specs=[hbm, hbm, hbm, vmem, hbm, hbm, smem],
        out_specs=(hbm, smem, hbm),
        scratch_shapes=[
            pltpu.VMEM((count, 3, width, order), bf16),
            pltpu.VMEM((count, order, inner), bf16),
            pltpu.VMEM((count, inner, order), bf16),
            pltpu.VMEM((count, inner, modes), bf16),
            pltpu.VMEM((count, 3, width, order), bf16),
            pltpu.VMEM((count, inner, order), bf16),
            pltpu.VMEM((count, modes, order), f32),
            pltpu.VMEM((CHUNKS, lanes, count, part, width), f32),
            pltpu.VMEM((CHUNKS, lanes, count, part, width), f32),
            pltpu.VMEM((lanes * count, part, width), f32),
            pltpu.VMEM((CHUNKS, owners, slots, part, width), f32),
            pltpu.VMEM((8, LANE), jnp.int32),
            pltpu.VMEM((lanes, 8, LANE), jnp.int32),
            pltpu.VMEM((owners, lanes, 8, LANE), jnp.int32),
            pltpu.SMEM((lanes, 8, LANE), jnp.int32),
            pltpu.SMEM((owners, lanes, 1, LANE), jnp.int32),
            dma((5, count)),
            dma((CHUNKS, lanes)),
            dma((CHUNKS, lanes)),
            dma((CHUNKS,)),
            dma((CHUNKS,)),
            dma((CHUNKS,)),
            dma((lanes,)),
            dma((lanes,)),
            dma((owners,)),
            dma((owners,)),
            dma((2,)),
            dma((count,)),
            dma((3,)),
            dma((PIECES,)),
        ],
        compiler_params=pltpu.CompilerParams(
            collective_id=0, has_side_effects=True, vmem_limit_bytes=VMEM_LIMIT
        ),
        name="reduce_and_send",
    )(stiff_bb, stiff_bi, constraint_modes, interior_mass, fixed_modes, mass_bb, boundary_map)
    block = jax.ShapeDtypeStruct((BPO * BAND, part, width), f32)
    k_out, m_out, coupling = pl.pallas_call(
        functools.partial(assemble, owners, slots),
        out_shape=(block, block, jax.ShapeDtypeStruct(coupled.shape, f32)),
        in_specs=[smem, hbm, hbm],
        out_specs=(hbm, hbm, hbm),
        scratch_shapes=[
            pltpu.VMEM(got.shape, f32),
            pltpu.VMEM((KINDS, BPO * BAND + 1, part, width), f32),
            pltpu.VMEM(coupled.shape, f32),
            dma((CHUNKS,)),
            dma((KINDS,)),
            dma((2,)),
        ],
        compiler_params=pltpu.CompilerParams(vmem_limit_bytes=VMEM_LIMIT),
        name="assemble",
    )(targets, got, coupled)
    shape = (BPO, BAND, part, width)
    return k_out.reshape(shape), m_out.reshape(shape), coupling


def solution(mesh):
    placed = (
        P(("row", "col"), None, None, None),
        P(("row", "col"), None, None),
        P(("row", "col"), None, None),
        P(("row", "col"), None),
        P(("row", "col"), None, None),
        P(("row", "col"), None, None, None),
        P(("row", "col"), None),
    )
    return jax.shard_map(
        per_device,
        mesh=mesh,
        in_specs=placed,
        out_specs=(
            P("row", None, "col", None),
            P("row", None, "col", None),
            P(("row", "col"), None, None),
        ),
        check_vma=False,
    )
```

```python
import functools
import jax
import jax.numpy as jnp
from jax import lax
from jax.experimental import pallas as pl
from jax.experimental.pallas import tpu as pltpu
from jax.sharding import PartitionSpec as P

BAND = 4
BPO = 24
LANE = 128

PAIRS = ((0, 0), (0, 1), (1, 1), (1, 2), (2, 2), (0, 2))
KINDS = 2
SPLIT = 1
CHUNKS = KINDS * len(PAIRS) * SPLIT
AHEAD = 2
LEAD = 4
PIECES = 4
MESH = pl.DeviceIdType.MESH
VMEM_LIMIT = 46 * 1024 * 1024
BAND_LIMIT = 12 * 1024 * 1024


def at_col(z):
    return {"row": lax.axis_index("row"), "col": z}


def at_row(r):
    return {"row": r, "col": lax.axis_index("col")}


def reduce_and_send(
    owners, lanes, slots,
    kbb, kbi, psi, mass, modes, mbb, table,
    got, targets, coupled,
    kbb_v, kbi_v, psi_v, modes_v, mbb_v, mass_v, weighted,
    reduced, grouped, staging, outgoing, table_v, maps_v, all_v, table_s, maps_s, all_s,
    load_sems, z_send, z_recv, r_sems, map_sems, small, block_sems,
):
    count, order, inner = kbi.shape
    width = order // 3
    part = width // lanes
    rows = part // SPLIT
    members = count * lanes
    row = lax.axis_index("row")
    col = lax.axis_index("col")

    def block_load(i):
        span = pl.ds(i * width, width)
        return pltpu.make_async_copy(kbi.at[0, span], kbi_v.at[0, span], block_sems.at[i])

    def piece_load(k):
        span = pl.ds(k * (inner // PIECES), inner // PIECES)
        return pltpu.make_async_copy(psi.at[0, span], psi_v.at[0, span], load_sems.at[1, 0])

    def loads(s):
        return (
            pltpu.make_async_copy(kbi.at[s], kbi_v.at[s], load_sems.at[0, s]),
            pltpu.make_async_copy(psi.at[s], psi_v.at[s], load_sems.at[1, s]),
        )

    first_kbb = pltpu.make_async_copy(kbb.at[0], kbb_v.at[0], small.at[0])
    others = pl.ds(1, count - 1)
    other_kbb = pltpu.make_async_copy(kbb.at[others], kbb_v.at[others], small.at[1])
    late_loads = (
        pltpu.make_async_copy(mass, mass_v, small.at[2]),
        pltpu.make_async_copy(mbb, mbb_v, small.at[3]),
        pltpu.make_async_copy(modes, modes_v, small.at[4]),
    )

    table_load = pltpu.make_async_copy(table, table_s, small.at[5])
    table_load.start()
    block_load(0).start()
    for k in range(PIECES):
        piece_load(k).start()
    first_kbb.start()
    for i in range(1, 3):
        block_load(i).start()

    barrier = pltpu.get_barrier_semaphore()
    for i in range(1, lanes):
        pl.semaphore_signal(barrier, inc=1, device_id=at_col(lax.rem(col + i, lanes)), device_id_type=MESH)

    def greet(i, carry):
        pl.semaphore_signal(barrier, inc=1, device_id=at_row(lax.rem(row + i, owners)), device_id_type=MESH)
        return carry

    lax.fori_loop(1, owners, greet, 0)

    def put(kind, s, i, strip):
        for j in range(i, 3):
            block = strip[:, (j - i) * width : (j - i + 1) * width].reshape(lanes, SPLIT, rows, width)
            for h in range(SPLIT):
                reduced[(kind * len(PAIRS) + PAIRS.index((i, j))) * SPLIT + h, :, s] = block[:, h]

    def stiff(s, i):
        strip = jnp.dot(
            kbi_v[s, i * width : (i + 1) * width, :], psi_v[s, :, i * width :],
            preferred_element_type=jnp.float32,
        )
        put(0, s, i, strip + kbb_v[s, i, :, i * width :].astype(jnp.float32))

    def drain(ref, sem):
        pltpu.make_async_copy(ref, ref, sem).wait()

    def z_map(i):
        return pltpu.make_async_remote_copy(
            src_ref=table_v, dst_ref=maps_v.at[col],
            send_sem=map_sems.at[0], recv_sem=map_sems.at[1],
            device_id=at_col(lax.rem(col + i, lanes)), device_id_type=MESH,
        )

    def z_copy(p, i):
        to = lax.rem(col + i, lanes)
        return pltpu.make_async_remote_copy(
            src_ref=reduced.at[p, to], dst_ref=grouped.at[p, col],
            send_sem=z_send, recv_sem=z_recv.at[p],
            device_id=at_col(to), device_id_type=MESH,
        )

    def z_copy_part(p, first, size, i):
        to = lax.rem(col + i, lanes)
        return pltpu.make_async_remote_copy(
            src_ref=reduced.at[p, to, pl.ds(first, size)], dst_ref=grouped.at[p, col, pl.ds(first, size)],
            send_sem=z_send, recv_sem=z_recv.at[p],
            device_id=at_col(to), device_id_type=MESH,
        )

    def r_map(i):
        return pltpu.make_async_remote_copy(
            src_ref=maps_v, dst_ref=all_v.at[row],
            send_sem=map_sems.at[2], recv_sem=map_sems.at[3],
            device_id=at_row(lax.rem(row + i, owners)), device_id_type=MESH,
        )

    half = CHUNKS // KINDS
    table_load.wait()
    place = (lax.broadcasted_iota(jnp.int32, (8, LANE), 0), lax.broadcasted_iota(jnp.int32, (8, LANE), 1))
    tile = jnp.zeros((8, LANE), jnp.int32)
    for s in range(count):
        for k in range(3):
            tile = jnp.where((place[0] == 0) & (place[1] == 3 * s + k), table_s[s, k], tile)
    table_v[...] = tile
    maps_v[col] = tile

    loads(0)[1].wait()
    first_kbb.wait()
    for i in range(3):
        block_load(i).wait()
        if i == 0:
            for later in range(1, count):
                for copy in loads(later):
                    copy.start()
            other_kbb.start()
            for copy in late_loads:
                copy.start()
        stiff(0, i)
        if i == 0:
            pl.semaphore_wait(barrier, lanes - 1 + owners - 1)
            for k in range(1, lanes):
                z_map(k).start()
        for j in range(i, 3):
            for h in range(SPLIT):
                for k in range(1, lanes):
                    z_copy_part(PAIRS.index((i, j)) * SPLIT + h, 0, 1, k).start()

    other_kbb.wait()

    def stiffs(s, carry):
        for copy in loads(s):
            copy.wait()
        for i in range(3):
            stiff(s, i)
        return carry

    lax.fori_loop(1, count, stiffs, 0)

    def send_rest(p):
        for i in range(1, lanes):
            z_copy_part(p, 1, count - 1, i).start()

    def send_chunk(p):
        for i in range(1, lanes):
            z_copy(p, i).start()

    for p in range(LEAD):
        send_rest(p)

    def masses(s, carry):
        pick = lax.broadcasted_iota(jnp.int32, (count, inner), 0) == s
        line = jnp.sum(jnp.where(pick, mass_v[...], 0.0), axis=0, keepdims=True)
        steps = inner // LANE
        lines = [line[:, k * LANE : (k + 1) * LANE] for k in range(steps)]
        filler = jnp.zeros((-steps % LANE, LANE), jnp.float32)
        columns = jnp.concatenate(lines + [filler], axis=0).T
        for k in range(steps):
            span = pl.ds(k * LANE, LANE)
            scale = jnp.broadcast_to(columns[:, k : k + 1], (LANE, order))
            weighted[s, span, :] = (scale * psi_v[s, span, :].astype(jnp.float32)).astype(jnp.bfloat16)
        for i in range(3):
            strip = lax.dot_general(
                psi_v[s, :, i * width : (i + 1) * width], weighted[s, :, i * width :], across,
                preferred_element_type=jnp.float32,
            )
            put(1, s, i, strip + mbb_v[s, i, :, i * width :].astype(jnp.float32))
        return carry

    across = (((0,), (0,)), ((), ()))
    for copy in late_loads:
        copy.wait()
    lax.fori_loop(0, count, masses, 0)

    for k in range(2):
        drain(maps_v.at[pl.ds(0, lanes - 1)], map_sems.at[k])
    to_scalar = pltpu.make_async_copy(maps_v, maps_s, small.at[6])
    to_scalar.start()
    lax.fori_loop(1, owners, lambda i, c: (r_map(i).start(), c)[1], 0)
    all_v[row] = maps_v[...]

    def couple(s, carry):
        coupled[s] = lax.dot_general(modes_v[s], weighted[s], across, preferred_element_type=jnp.float32)
        return carry

    def keep(p, carry):
        grouped[p, col] = reduced[p, col]
        return carry

    lax.fori_loop(0, CHUNKS, keep, 0)
    lax.fori_loop(0, count, couple, 0)

    to_scalar.wait()

    belongs = [maps_s[m // count, 0, 3 * (m % count)] // BPO for m in range(members)]
    ranks = []
    for m in range(members):
        rank = jnp.int32(0)
        for e in range(m):
            rank = rank + jnp.where(belongs[e] == belongs[m], 1, 0)
        ranks.append(rank)
    places = [belongs[m] * slots + ranks[m] for m in range(members)]

    chosen = []
    for slot in range(owners * slots):
        member = jnp.int32(0)
        for m in range(1, members):
            member = jnp.where(places[m] == slot, m, member)
        chosen.append(member)

    def forward(send, p, carry):
        drain(grouped.at[p, pl.ds(0, lanes - 1)], z_recv.at[p])
        if send is not None:
            send(p)

        staging[...] = grouped[p].reshape(members, rows, width)
        for slot, member in enumerate(chosen):
            outgoing[p, slot // slots, slot % slots] = staging[member]

        def ship(i, inner_carry):
            r_copy(p, i).start()
            return inner_carry

        lax.fori_loop(1, owners, ship, 0)
        got[p, row] = outgoing[p, row]
        return carry

    def r_copy(p, i):
        to = lax.rem(row + i, owners)
        return pltpu.make_async_remote_copy(
            src_ref=outgoing.at[p, to], dst_ref=got.at[p, row],
            send_sem=r_sems.at[0], recv_sem=r_sems.at[1],
            device_id=at_row(to), device_id_type=MESH,
        )

    for k in range(2, 4):
        drain(all_v.at[pl.ds(0, owners - 1)], map_sems.at[k])
    all_scalar = pltpu.make_async_copy(all_v.at[:, :, pl.ds(0, 1)], all_s, small.at[7])
    all_scalar.start()
    all_scalar.wait()

    def aim(group, carry):
        picked = [[jnp.int32(-1)] * 3 for _ in range(slots)]
        filled = jnp.int32(0)
        for m in range(members):
            at = [all_s[group, m // count, 0, 3 * (m % count) + k] for k in range(3)]
            mine = at[0] // BPO == row
            for slot in range(slots):
                hit = mine & (filled == slot)
                picked[slot] = [jnp.where(hit, at[k], picked[slot][k]) for k in range(3)]
            filled = filled + jnp.where(mine, 1, 0)
        for slot in range(slots):
            at = picked[slot]
            for p, (i, j) in enumerate(PAIRS):
                local = (at[i] - row * BPO) * BAND + at[j] - at[i]
                targets[p, group * slots + slot] = jnp.where(at[0] >= 0, local, BPO * BAND)
        return carry

    lax.fori_loop(0, owners, aim, 0)
    def follow(first, last, send):
        lax.fori_loop(first, last, functools.partial(forward, send), 0)

    follow(0, half - LEAD, lambda p: send_rest(p + LEAD))
    follow(half - LEAD, half - AHEAD, None)
    follow(half - AHEAD, CHUNKS - AHEAD, lambda p: send_chunk(p + AHEAD))
    follow(CHUNKS - AHEAD, CHUNKS, None)

    drain(grouped.at[:, pl.ds(0, lanes - 1)], z_send)
    for k in range(2):
        drain(got.at[:, pl.ds(0, owners - 1)], r_sems.at[k])


def assemble(owners, slots, targets, got, coupled, k_out, m_out, coupling, band, out_sems):
    limit = BPO * BAND
    writes = [pltpu.make_async_copy(coupled, coupling, out_sems.at[KINDS])]
    writes[0].start()
    for kind, out in enumerate((k_out, m_out)):
        band[kind] = jnp.zeros(band.shape[1:], band.dtype)
        for p in range(len(PAIRS)):
            chunk = pl.ds((kind * len(PAIRS) + p) * SPLIT, SPLIT)
            for place in range(owners * slots):
                at = targets[p, place]
                band[kind, at] += got[chunk, place // slots, place % slots].reshape(band.shape[2:])
        writes.append(pltpu.make_async_copy(band.at[kind, pl.ds(0, limit)], out, out_sems.at[kind]))
        writes[-1].start()
    for write in writes:
        write.wait()


def per_device(
    stiff_bb, stiff_bi, constraint_modes, interior_mass, fixed_modes, mass_bb, boundary_map
):
    owners = lax.axis_size("row")
    lanes = lax.axis_size("col")
    count, order, inner = stiff_bi.shape
    modes = fixed_modes.shape[2]
    width = order // 3
    part = width // lanes
    rows = part // SPLIT
    slots = (count * lanes + owners - 1) // owners
    f32, bf16 = jnp.float32, jnp.bfloat16
    hbm = pl.BlockSpec(memory_space=pltpu.HBM)
    vmem = pl.BlockSpec(memory_space=pltpu.VMEM)
    smem = pl.BlockSpec(memory_space=pltpu.SMEM)
    dma = pltpu.SemaphoreType.DMA
    got, targets, coupled = pl.pallas_call(
        functools.partial(reduce_and_send, owners, lanes, slots),
        out_shape=(
            pltpu.VMEM((CHUNKS, owners, slots, rows, width), f32),
            jax.ShapeDtypeStruct((len(PAIRS), owners * slots), jnp.int32),
            pltpu.VMEM((count, modes, order), f32),
        ),
        in_specs=[hbm] * 7,
        out_specs=(vmem, smem, vmem),
        scratch_shapes=[
            pltpu.VMEM((count, 3, width, order), bf16),
            pltpu.VMEM((count, order, inner), bf16),
            pltpu.VMEM((count, inner, order), bf16),
            pltpu.VMEM((count, inner, modes), bf16),
            pltpu.VMEM((count, 3, width, order), bf16),
            pltpu.VMEM((count, inner), f32),
            pltpu.VMEM((count, inner, order), bf16),
            pltpu.VMEM((CHUNKS, lanes, count, rows, width), f32),
            pltpu.VMEM((CHUNKS, lanes, count, rows, width), f32),
            pltpu.VMEM((lanes * count, rows, width), f32),
            pltpu.VMEM((CHUNKS, owners, slots, rows, width), f32),
            pltpu.VMEM((8, LANE), jnp.int32),
            pltpu.VMEM((lanes, 8, LANE), jnp.int32),
            pltpu.VMEM((owners, lanes, 8, LANE), jnp.int32),
            pltpu.SMEM((count, 3), jnp.int32),
            pltpu.SMEM((lanes, 8, LANE), jnp.int32),
            pltpu.SMEM((owners, lanes, 1, LANE), jnp.int32),
            dma((2, count)),
            dma,
            dma((CHUNKS,)),
            dma((2,)),
            dma((4,)),
            dma((8,)),
            dma((3,)),
        ],
        compiler_params=pltpu.CompilerParams(
            collective_id=0, has_side_effects=True, vmem_limit_bytes=VMEM_LIMIT
        ),
        name="reduce_and_send",
    )(*(
        pltpu.with_memory_space_constraint(x, pltpu.HBM)
        for x in (stiff_bb, stiff_bi, constraint_modes, interior_mass, fixed_modes, mass_bb, boundary_map)
    ))
    block = jax.ShapeDtypeStruct((BPO * BAND, part, width), f32)
    k_out, m_out, coupling = pl.pallas_call(
        functools.partial(assemble, owners, slots),
        out_shape=(block, block, jax.ShapeDtypeStruct(coupled.shape, f32)),
        in_specs=[smem, vmem, vmem],
        out_specs=(hbm, hbm, hbm),
        scratch_shapes=[
            pltpu.VMEM((KINDS, BPO * BAND + 1, part, width), f32),
            dma((KINDS + 1,)),
        ],
        compiler_params=pltpu.CompilerParams(vmem_limit_bytes=BAND_LIMIT),
        name="assemble",
    )(targets, got, coupled)
    shape = (BPO, BAND, part, width)
    return k_out.reshape(shape), m_out.reshape(shape), coupling


def solution(mesh):
    placed = (
        P(("row", "col"), None, None, None),
        P(("row", "col"), None, None),
        P(("row", "col"), None, None),
        P(("row", "col"), None),
        P(("row", "col"), None, None),
        P(("row", "col"), None, None, None),
        P(("row", "col"), None),
    )
    return jax.shard_map(
        per_device,
        mesh=mesh,
        in_specs=placed,
        out_specs=(
            P("row", None, "col", None),
            P("row", None, "col", None),
            P(("row", "col"), None, None),
        ),
        check_vma=False,
    )
```

```python
import functools
import jax
import jax.numpy as jnp
from jax import lax
from jax.experimental import pallas as pl
from jax.experimental.pallas import tpu as pltpu
from jax.sharding import PartitionSpec as P

BAND = 4
BPO = 24
LANE = 128

PAIRS = ((0, 0), (0, 1), (1, 1), (1, 2), (2, 2), (0, 2))
KINDS = 2
SPLIT = 1
CHUNKS = KINDS * len(PAIRS) * SPLIT
AHEAD = 2
LEAD = 4
MESH = pl.DeviceIdType.MESH
VMEM_LIMIT = 55 * 1024 * 1024
BAND_LIMIT = 1024 * 1024


def at_col(z):
    return {"row": lax.axis_index("row"), "col": z}


def at_row(r):
    return {"row": r, "col": lax.axis_index("col")}


def reduce_and_send(
    owners, lanes, slots,
    kbb, kbi, psi, mass, modes, mbb, table,
    k_band, m_band, coupled,
    got, totals, targets, links_v, links_s,
    kbb_v, kbi_v, psi_v, modes_v, mbb_v, mass_v, weighted,
    reduced, grouped, staging, outgoing, table_v, maps_v, all_v, table_s, maps_s, all_s,
    load_sems, z_send, z_recv, r_sems, map_sems, small, block_sems,
):
    count, order, inner = kbi.shape
    width = order // 3
    part = width // lanes
    rows = part // SPLIT
    members = count * lanes
    row = lax.axis_index("row")
    col = lax.axis_index("col")

    def block_load(i):
        span = pl.ds(i * width, width)
        return (
            pltpu.make_async_copy(kbi.at[0, span], kbi_v.at[0, span], block_sems.at[0, i]),
            pltpu.make_async_copy(psi.at[0, :, span], psi_v.at[0, :, span], block_sems.at[1, i]),
        )

    def loads(s):
        return (
            pltpu.make_async_copy(kbi.at[s], kbi_v.at[s], load_sems.at[0, s]),
            pltpu.make_async_copy(psi.at[s], psi_v.at[s], load_sems.at[1, s]),
        )

    first_kbb = pltpu.make_async_copy(kbb.at[0], kbb_v.at[0], small.at[0])
    others = pl.ds(1, count - 1)
    other_kbb = pltpu.make_async_copy(kbb.at[others], kbb_v.at[others], small.at[1])
    late_loads = (
        pltpu.make_async_copy(mass, mass_v, small.at[2]),
        pltpu.make_async_copy(mbb, mbb_v, small.at[3]),
        pltpu.make_async_copy(modes, modes_v, small.at[4]),
    )

    for copy in block_load(2):
        copy.start()
    first_kbb.start()
    table_load = pltpu.make_async_copy(table, table_s, small.at[5])
    table_load.start()

    barrier = pltpu.get_barrier_semaphore()
    for i in range(1, lanes):
        pl.semaphore_signal(barrier, inc=1, device_id=at_col(lax.rem(col + i, lanes)), device_id_type=MESH)

    def greet(i, carry):
        pl.semaphore_signal(barrier, inc=1, device_id=at_row(lax.rem(row + i, owners)), device_id_type=MESH)
        return carry

    lax.fori_loop(1, owners, greet, 0)

    def put(kind, s, i, strip):
        for j in range(i, 3):
            block = strip[:, (j - i) * width : (j - i + 1) * width].reshape(lanes, SPLIT, rows, width)
            for h in range(SPLIT):
                reduced[(kind * len(PAIRS) + PAIRS.index((i, j))) * SPLIT + h, :, s] = block[:, h]

    def stiff(s, i):
        strip = jnp.dot(
            kbi_v[s, i * width : (i + 1) * width, :], psi_v[s, :, i * width :],
            preferred_element_type=jnp.float32,
        )
        put(0, s, i, strip + kbb_v[s, i, :, i * width :].astype(jnp.float32))

    def drain(ref, sem):
        pltpu.make_async_copy(ref, ref, sem).wait()

    def z_map(i):
        return pltpu.make_async_remote_copy(
            src_ref=table_v, dst_ref=maps_v.at[col],
            send_sem=map_sems.at[0], recv_sem=map_sems.at[1],
            device_id=at_col(lax.rem(col + i, lanes)), device_id_type=MESH,
        )

    def z_copy(p, i):
        to = lax.rem(col + i, lanes)
        return pltpu.make_async_remote_copy(
            src_ref=reduced.at[p, to], dst_ref=grouped.at[p, col],
            send_sem=z_send, recv_sem=z_recv.at[p],
            device_id=at_col(to), device_id_type=MESH,
        )

    def z_copy_part(p, first, size, i):
        to = lax.rem(col + i, lanes)
        return pltpu.make_async_remote_copy(
            src_ref=reduced.at[p, to, pl.ds(first, size)], dst_ref=grouped.at[p, col, pl.ds(first, size)],
            send_sem=z_send, recv_sem=z_recv.at[p],
            device_id=at_col(to), device_id_type=MESH,
        )

    def r_map(i):
        return pltpu.make_async_remote_copy(
            src_ref=maps_v, dst_ref=all_v.at[row],
            send_sem=map_sems.at[2], recv_sem=map_sems.at[3],
            device_id=at_row(lax.rem(row + i, owners)), device_id_type=MESH,
        )

    half = CHUNKS // KINDS
    table_load.wait()
    for i in (1, 0):
        for copy in block_load(i):
            copy.start()
    place = (lax.broadcasted_iota(jnp.int32, (8, LANE), 0), lax.broadcasted_iota(jnp.int32, (8, LANE), 1))
    tile = jnp.zeros((8, LANE), jnp.int32)
    for s in range(count):
        for k in range(3):
            tile = jnp.where((place[0] == 0) & (place[1] == 3 * s + k), table_s[s, k], tile)
    table_v[...] = tile
    maps_v[col] = tile

    first_kbb.wait()
    for i in reversed(range(3)):
        for copy in block_load(i):
            copy.wait()
        if i == 1:
            for later in range(1, count):
                for copy in loads(later):
                    copy.start()
            other_kbb.start()
            for copy in late_loads:
                copy.start()
        stiff(0, i)
        if i == 2:
            pl.semaphore_wait(barrier, lanes - 1 + owners - 1)
            for k in range(1, lanes):
                z_map(k).start()
        for j in range(i, 3):
            for h in range(SPLIT):
                for k in range(1, lanes):
                    z_copy_part(PAIRS.index((i, j)) * SPLIT + h, 0, 1, k).start()

    other_kbb.wait()

    def stiffs(s, carry):
        for copy in loads(s):
            copy.wait()
        for i in range(3):
            stiff(s, i)
        return carry

    lax.fori_loop(1, count, stiffs, 0)

    def send_rest(p):
        for i in range(1, lanes):
            z_copy_part(p, 1, count - 1, i).start()

    def send_chunk(p):
        for i in range(1, lanes):
            z_copy(p, i).start()

    for p in range(LEAD):
        send_rest(p)

    def masses(s, carry):
        pick = lax.broadcasted_iota(jnp.int32, (count, inner), 0) == s
        line = jnp.sum(jnp.where(pick, mass_v[...], 0.0), axis=0, keepdims=True)
        steps = inner // LANE
        lines = [line[:, k * LANE : (k + 1) * LANE] for k in range(steps)]
        filler = jnp.zeros((-steps % LANE, LANE), jnp.float32)
        columns = jnp.concatenate(lines + [filler], axis=0).T
        for k in range(steps):
            span = pl.ds(k * LANE, LANE)
            scale = jnp.broadcast_to(columns[:, k : k + 1], (LANE, order))
            weighted[s, span, :] = (scale * psi_v[s, span, :].astype(jnp.float32)).astype(jnp.bfloat16)
        for i in range(3):
            strip = lax.dot_general(
                psi_v[s, :, i * width : (i + 1) * width], weighted[s, :, i * width :], across,
                preferred_element_type=jnp.float32,
            )
            put(1, s, i, strip + mbb_v[s, i, :, i * width :].astype(jnp.float32))
        return carry

    across = (((0,), (0,)), ((), ()))
    for copy in late_loads:
        copy.wait()
    lax.fori_loop(0, count, masses, 0)

    for k in range(2):
        drain(maps_v.at[pl.ds(0, lanes - 1)], map_sems.at[k])
    to_scalar = pltpu.make_async_copy(maps_v, maps_s, small.at[6])
    to_scalar.start()
    lax.fori_loop(1, owners, lambda i, c: (r_map(i).start(), c)[1], 0)
    all_v[row] = maps_v[...]

    def couple(s, carry):
        coupled[s] = lax.dot_general(modes_v[s], weighted[s], across, preferred_element_type=jnp.float32)
        return carry

    def keep(p, carry):
        grouped[p, col] = reduced[p, col]
        return carry

    lax.fori_loop(0, CHUNKS, keep, 0)
    lax.fori_loop(0, count, couple, 0)

    to_scalar.wait()

    belongs = [maps_s[m // count, 0, 3 * (m % count)] // BPO for m in range(members)]
    ranks = []
    for m in range(members):
        rank = jnp.int32(0)
        for e in range(m):
            rank = rank + jnp.where(belongs[e] == belongs[m], 1, 0)
        ranks.append(rank)
    places = [belongs[m] * slots + ranks[m] for m in range(members)]

    chosen = []
    for slot in range(owners * slots):
        member = jnp.int32(0)
        for m in range(1, members):
            member = jnp.where(places[m] == slot, m, member)
        chosen.append(member)

    def forward(send, p, carry):
        drain(grouped.at[p, pl.ds(0, lanes - 1)], z_recv.at[p])
        if send is not None:
            send(p)

        staging[...] = grouped[p].reshape(members, rows, width)
        for slot, member in enumerate(chosen):
            outgoing[p, slot // slots, slot % slots] = staging[member]

        def ship(i, inner_carry):
            r_copy(p, i).start()
            return inner_carry

        lax.fori_loop(1, owners, ship, 0)
        got[p, row] = outgoing[p, row]
        return carry

    def arrival(p):
        return jnp.where(p < half, 1, jnp.where(p < CHUNKS - SPLIT, 2, 3))

    def r_copy(p, i):
        to = lax.rem(row + i, owners)
        return pltpu.make_async_remote_copy(
            src_ref=outgoing.at[p, to], dst_ref=got.at[p, row],
            send_sem=r_sems.at[0], recv_sem=r_sems.at[arrival(p)],
            device_id=at_row(to), device_id_type=MESH,
        )

    for k in range(2, 4):
        drain(all_v.at[pl.ds(0, owners - 1)], map_sems.at[k])
    all_scalar = pltpu.make_async_copy(all_v.at[:, :, pl.ds(0, 1)], all_s, small.at[7])
    all_scalar.start()
    all_scalar.wait()

    seats = owners * slots
    entries = len(PAIRS) * seats
    extent = entries + -entries % LANE
    limit = BPO * BAND

    def links():
        goals = [targets[c // seats, c % seats] for c in range(entries)]
        lane = lax.broadcasted_iota(jnp.int32, (8, extent), 1)
        sub = lax.broadcasted_iota(jnp.int32, (8, extent), 0)
        along = jnp.full((8, extent), -1, jnp.int32)
        for c in range(entries):
            along = jnp.where(lane == c, goals[c], along)
        before = jnp.full((8, extent), -1, jnp.int32)
        final = jnp.full((8, extent), -1, jnp.int32)
        for base in range(0, entries, 8):
            down = jnp.full((8, extent), -2, jnp.int32)
            for r in range(8):
                down = jnp.where(sub == r, goals[base + r], down)
            entry = sub + base
            before = jnp.where((down == along) & (entry < lane), entry, before)
            final = jnp.where(down == lane, entry, final)
        for kind, found in enumerate((before, final)):
            best = found[0:1]
            for r in range(1, 8):
                best = jnp.maximum(best, found[r : r + 1])
            links_v[kind : kind + 1] = jnp.where(best < 0, entries, best)
        to_links = pltpu.make_async_copy(links_v, links_s, small.at[6])
        to_links.start()
        to_links.wait()

    def chain(kind, p, carry):
        for seat in range(seats):
            c = p * seats + seat
            piece = got[pl.ds((kind * len(PAIRS) + p) * SPLIT, SPLIT), seat // slots, seat % slots]
            totals[kind, c] = piece.reshape(part, width) + totals[kind, links_s[0, c]]
        return carry

    def aim(group, carry):
        picked = [[jnp.int32(-1)] * 3 for _ in range(slots)]
        filled = jnp.int32(0)
        for m in range(members):
            at = [all_s[group, m // count, 0, 3 * (m % count) + k] for k in range(3)]
            mine = at[0] // BPO == row
            for slot in range(slots):
                hit = mine & (filled == slot)
                picked[slot] = [jnp.where(hit, at[k], picked[slot][k]) for k in range(3)]
            filled = filled + jnp.where(mine, 1, 0)
        for slot in range(slots):
            at = picked[slot]
            for p, (i, j) in enumerate(PAIRS):
                local = (at[i] - row * BPO) * BAND + at[j] - at[i]
                targets[p, group * slots + slot] = jnp.where(at[0] >= 0, local, BPO * BAND)
        return carry

    lax.fori_loop(0, owners, aim, 0)
    links()

    def follow(first, last, send):
        lax.fori_loop(first, last, functools.partial(forward, send), 0)

    follow(0, half - LEAD, lambda p: send_rest(p + LEAD))
    follow(half - LEAD, half - AHEAD, None)
    follow(half - AHEAD, CHUNKS - AHEAD, lambda p: send_chunk(p + AHEAD))
    follow(CHUNKS - AHEAD, CHUNKS, None)

    def arrived(first, last, k):
        drain(got.at[pl.ds(first, last - first), pl.ds(0, owners - 1)], r_sems.at[k])

    def gather(kind, band, first, last):
        def row_block(g, carry):
            for d in range(first, last):
                band[g * BAND + d] = totals[kind, links_s[1, g * BAND + d]]
            return carry

        lax.fori_loop(0, BPO, row_block, 0)

    for kind in range(KINDS):
        totals[kind, entries] = jnp.zeros((part, width), jnp.float32)
    arrived(0, half, 1)
    lax.fori_loop(0, len(PAIRS), functools.partial(chain, 0), 0)
    gather(0, k_band, 0, BAND)
    arrived(half, CHUNKS - SPLIT, 2)
    lax.fori_loop(0, len(PAIRS) - 1, functools.partial(chain, 1), 0)
    gather(1, m_band, 0, 2)
    drain(grouped.at[:, pl.ds(0, lanes - 1)], z_send)
    arrived(CHUNKS - SPLIT, CHUNKS, 3)
    chain(1, len(PAIRS) - 1, 0)
    gather(1, m_band, 2, BAND)
    drain(got.at[:, pl.ds(0, owners - 1)], r_sems.at[0])


def hand_out(k_band, m_band, coupled, k_out, m_out, coupling, sems):
    writes = [
        pltpu.make_async_copy(source, out, sems.at[i])
        for i, (source, out) in enumerate(((k_band, k_out), (m_band, m_out), (coupled, coupling)))
    ]
    for write in writes:
        write.start()
    for write in writes:
        write.wait()


def per_device(
    stiff_bb, stiff_bi, constraint_modes, interior_mass, fixed_modes, mass_bb, boundary_map
):
    owners = lax.axis_size("row")
    lanes = lax.axis_size("col")
    count, order, inner = stiff_bi.shape
    modes = fixed_modes.shape[2]
    width = order // 3
    part = width // lanes
    rows = part // SPLIT
    slots = (count * lanes + owners - 1) // owners
    f32, bf16 = jnp.float32, jnp.bfloat16
    hbm = pl.BlockSpec(memory_space=pltpu.HBM)
    vmem = pl.BlockSpec(memory_space=pltpu.VMEM)
    dma = pltpu.SemaphoreType.DMA
    seats = owners * slots
    entries = len(PAIRS) * seats
    extent = entries + -entries % LANE
    band = pltpu.VMEM((BPO * BAND, part, width), f32)
    bands = pl.pallas_call(
        functools.partial(reduce_and_send, owners, lanes, slots),
        out_shape=(
            band,
            band,
            pltpu.VMEM((count, modes, order), f32),
        ),
        in_specs=[hbm] * 7,
        out_specs=(vmem, vmem, vmem),
        scratch_shapes=[
            pltpu.VMEM((CHUNKS, owners, slots, rows, width), f32),
            pltpu.VMEM((KINDS, entries + 1, part, width), f32),
            pltpu.SMEM((len(PAIRS), seats), jnp.int32),
            pltpu.VMEM((KINDS, extent), jnp.int32),
            pltpu.SMEM((KINDS, extent), jnp.int32),
            pltpu.VMEM((count, 3, width, order), bf16),
            pltpu.VMEM((count, order, inner), bf16),
            pltpu.VMEM((count, inner, order), bf16),
            pltpu.VMEM((count, inner, modes), bf16),
            pltpu.VMEM((count, 3, width, order), bf16),
            pltpu.VMEM((count, inner), f32),
            pltpu.VMEM((count, inner, order), bf16),
            pltpu.VMEM((CHUNKS, lanes, count, rows, width), f32),
            pltpu.VMEM((CHUNKS, lanes, count, rows, width), f32),
            pltpu.VMEM((lanes * count, rows, width), f32),
            pltpu.VMEM((CHUNKS, owners, slots, rows, width), f32),
            pltpu.VMEM((8, LANE), jnp.int32),
            pltpu.VMEM((lanes, 8, LANE), jnp.int32),
            pltpu.VMEM((owners, lanes, 8, LANE), jnp.int32),
            pltpu.SMEM((count, 3), jnp.int32),
            pltpu.SMEM((lanes, 8, LANE), jnp.int32),
            pltpu.SMEM((owners, lanes, 1, LANE), jnp.int32),
            dma((2, count)),
            dma,
            dma((CHUNKS,)),
            dma((4,)),
            dma((4,)),
            dma((8,)),
            dma((2, 3)),
        ],
        compiler_params=pltpu.CompilerParams(
            collective_id=0, has_side_effects=True, vmem_limit_bytes=VMEM_LIMIT
        ),
        name="reduce_and_send",
    )(*(
        pltpu.with_memory_space_constraint(x, pltpu.HBM)
        for x in (stiff_bb, stiff_bi, constraint_modes, interior_mass, fixed_modes, mass_bb, boundary_map)
    ))
    block = jax.ShapeDtypeStruct(band.shape, f32)
    k_out, m_out, coupling = pl.pallas_call(
        hand_out,
        out_shape=(block, block, jax.ShapeDtypeStruct((count, modes, order), f32)),
        in_specs=[vmem] * 3,
        out_specs=(hbm, hbm, hbm),
        scratch_shapes=[dma((3,))],
        compiler_params=pltpu.CompilerParams(vmem_limit_bytes=BAND_LIMIT),
        name="hand_out",
    )(*bands)
    shape = (BPO, BAND, part, width)
    return k_out.reshape(shape), m_out.reshape(shape), coupling


def solution(mesh):
    placed = (
        P(("row", "col"), None, None, None),
        P(("row", "col"), None, None),
        P(("row", "col"), None, None),
        P(("row", "col"), None),
        P(("row", "col"), None, None),
        P(("row", "col"), None, None, None),
        P(("row", "col"), None),
    )
    return jax.shard_map(
        per_device,
        mesh=mesh,
        in_specs=placed,
        out_specs=(
            P("row", None, "col", None),
            P("row", None, "col", None),
            P(("row", "col"), None, None),
        ),
        check_vma=False,
    )
```

```python
import functools
import jax
import jax.numpy as jnp
from jax import lax
from jax.experimental import pallas as pl
from jax.experimental.pallas import tpu as pltpu
from jax.sharding import PartitionSpec as P

BAND = 4
BPO = 24
LANE = 128

PAIRS = ((0, 0), (0, 1), (1, 1), (1, 2), (2, 2), (0, 2))
KINDS = 2
SPLIT = 1
CHUNKS = KINDS * len(PAIRS) * SPLIT
AHEAD = 2
LEAD = 4
TURN = 3
MESH = pl.DeviceIdType.MESH
VMEM_LIMIT = 55 * 1024 * 1024
BAND_LIMIT = 1024 * 1024


def at_col(z):
    return {"row": lax.axis_index("row"), "col": z}


def at_row(r):
    return {"row": r, "col": lax.axis_index("col")}


def reduce_and_send(
    owners, lanes, slots,
    kbb, kbi, psi, mass, modes, mbb, table,
    k_band, m_band, coupled,
    got, totals, targets, links_v, links_s,
    kbb_v, kbi_v, psi_v, modes_v, mbb_v, mass_v, weighted,
    reduced, grouped, staging, outgoing, table_v, maps_v, all_v, table_s, maps_s, all_s,
    load_sems, z_send, z_recv, r_sems, map_sems, small, block_sems,
):
    count, order, inner = kbi.shape
    width = order // 3
    part = width // lanes
    rows = part // SPLIT
    members = count * lanes
    row = lax.axis_index("row")
    col = lax.axis_index("col")

    def block_load(i):
        span = pl.ds(i * width, width)
        return (
            pltpu.make_async_copy(kbi.at[0, span], kbi_v.at[0, span], block_sems.at[0, i]),
            pltpu.make_async_copy(psi.at[0, :, span], psi_v.at[0, :, span], block_sems.at[1, i]),
        )

    def loads(s):
        return (
            pltpu.make_async_copy(kbi.at[s], kbi_v.at[s], load_sems.at[0, s]),
            pltpu.make_async_copy(psi.at[s], psi_v.at[s], load_sems.at[1, s]),
        )

    first_kbb = pltpu.make_async_copy(kbb.at[0], kbb_v.at[0], small.at[0])
    others = pl.ds(1, count - 1)
    other_kbb = pltpu.make_async_copy(kbb.at[others], kbb_v.at[others], small.at[1])
    late_loads = (
        pltpu.make_async_copy(mass, mass_v, small.at[2]),
        pltpu.make_async_copy(mbb, mbb_v, small.at[3]),
        pltpu.make_async_copy(modes, modes_v, small.at[4]),
    )

    for copy in block_load(2):
        copy.start()
    first_kbb.start()
    table_load = pltpu.make_async_copy(table, table_s, small.at[5])
    table_load.start()

    barrier = pltpu.get_barrier_semaphore()
    for i in range(1, lanes):
        pl.semaphore_signal(barrier, inc=1, device_id=at_col(lax.rem(col + i, lanes)), device_id_type=MESH)

    def greet(i, carry):
        pl.semaphore_signal(barrier, inc=1, device_id=at_row(lax.rem(row + i, owners)), device_id_type=MESH)
        return carry

    lax.fori_loop(1, owners, greet, 0)

    def put(kind, s, i, strip):
        for j in range(i, 3):
            block = strip[:, (j - i) * width : (j - i + 1) * width].reshape(lanes, SPLIT, rows, width)
            for h in range(SPLIT):
                reduced[(kind * len(PAIRS) + PAIRS.index((i, j))) * SPLIT + h, :, s] = block[:, h]

    def stiff(s, i):
        strip = jnp.dot(
            kbi_v[s, i * width : (i + 1) * width, :], psi_v[s, :, i * width :],
            preferred_element_type=jnp.float32,
        )
        put(0, s, i, strip + kbb_v[s, i, :, i * width :].astype(jnp.float32))

    def drain(ref, sem):
        pltpu.make_async_copy(ref, ref, sem).wait()

    def z_map(i):
        return pltpu.make_async_remote_copy(
            src_ref=table_v, dst_ref=maps_v.at[col],
            send_sem=map_sems.at[0], recv_sem=map_sems.at[1],
            device_id=at_col(lax.rem(col + i, lanes)), device_id_type=MESH,
        )

    def z_copy(p, i):
        to = lax.rem(col + i, lanes)
        return pltpu.make_async_remote_copy(
            src_ref=reduced.at[p, to], dst_ref=grouped.at[p, col],
            send_sem=z_send, recv_sem=z_recv.at[p],
            device_id=at_col(to), device_id_type=MESH,
        )

    def z_copy_part(p, first, size, i):
        to = lax.rem(col + i, lanes)
        return pltpu.make_async_remote_copy(
            src_ref=reduced.at[p, to, pl.ds(first, size)], dst_ref=grouped.at[p, col, pl.ds(first, size)],
            send_sem=z_send, recv_sem=z_recv.at[p],
            device_id=at_col(to), device_id_type=MESH,
        )

    def r_map(i):
        return pltpu.make_async_remote_copy(
            src_ref=maps_v, dst_ref=all_v.at[row],
            send_sem=map_sems.at[2], recv_sem=map_sems.at[3],
            device_id=at_row(lax.rem(row + i, owners)), device_id_type=MESH,
        )

    half = CHUNKS // KINDS
    table_load.wait()
    for i in (1, 0):
        for copy in block_load(i):
            copy.start()
    place = (lax.broadcasted_iota(jnp.int32, (8, LANE), 0), lax.broadcasted_iota(jnp.int32, (8, LANE), 1))
    tile = jnp.zeros((8, LANE), jnp.int32)
    for s in range(count):
        for k in range(3):
            tile = jnp.where((place[0] == 0) & (place[1] == 3 * s + k), table_s[s, k], tile)
    table_v[...] = tile
    maps_v[col] = tile

    first_kbb.wait()
    for i in reversed(range(3)):
        for copy in block_load(i):
            copy.wait()
        if i == 1:
            for later in range(1, count):
                for copy in loads(later):
                    copy.start()
            other_kbb.start()
            for copy in late_loads:
                copy.start()
        stiff(0, i)
        if i == 2:
            pl.semaphore_wait(barrier, lanes - 1 + owners - 1)
            for k in range(1, lanes):
                z_map(k).start()
        for j in range(i, 3):
            for h in range(SPLIT):
                for k in range(1, lanes):
                    z_copy_part(PAIRS.index((i, j)) * SPLIT + h, 0, 1, k).start()

    other_kbb.wait()

    def stiffs(s, carry):
        for copy in loads(s):
            copy.wait()
        for i in range(3):
            stiff(s, i)
        return carry

    lax.fori_loop(1, count, stiffs, 0)

    def send(p):
        @pl.when(p < half)
        def _():
            for k in range(1, lanes):
                z_copy_part(p, 1, count - 1, k).start()

        @pl.when(p >= half)
        def _():
            for k in range(1, lanes):
                z_copy(p, k).start()

    for p in range(LEAD):
        send(p)

    def masses(s, carry):
        pick = lax.broadcasted_iota(jnp.int32, (count, inner), 0) == s
        line = jnp.sum(jnp.where(pick, mass_v[...], 0.0), axis=0, keepdims=True)
        steps = inner // LANE
        lines = [line[:, k * LANE : (k + 1) * LANE] for k in range(steps)]
        filler = jnp.zeros((-steps % LANE, LANE), jnp.float32)
        columns = jnp.concatenate(lines + [filler], axis=0).T
        for k in range(steps):
            span = pl.ds(k * LANE, LANE)
            scale = jnp.broadcast_to(columns[:, k : k + 1], (LANE, order))
            weighted[s, span, :] = (scale * psi_v[s, span, :].astype(jnp.float32)).astype(jnp.bfloat16)
        for i in range(3):
            strip = lax.dot_general(
                psi_v[s, :, i * width : (i + 1) * width], weighted[s, :, i * width :], across,
                preferred_element_type=jnp.float32,
            )
            put(1, s, i, strip + mbb_v[s, i, :, i * width :].astype(jnp.float32))
        return carry

    across = (((0,), (0,)), ((), ()))
    for copy in late_loads:
        copy.wait()
    lax.fori_loop(0, count, masses, 0)

    for k in range(2):
        drain(maps_v.at[pl.ds(0, lanes - 1)], map_sems.at[k])
    to_scalar = pltpu.make_async_copy(maps_v, maps_s, small.at[6])
    to_scalar.start()
    lax.fori_loop(1, owners, lambda i, c: (r_map(i).start(), c)[1], 0)
    all_v[row] = maps_v[...]

    def couple(s, carry):
        coupled[s] = lax.dot_general(modes_v[s], weighted[s], across, preferred_element_type=jnp.float32)
        return carry

    def keep(p, carry):
        grouped[p, col] = reduced[p, col]
        return carry

    lax.fori_loop(0, CHUNKS, keep, 0)
    lax.fori_loop(0, count, couple, 0)

    to_scalar.wait()

    belongs = [maps_s[m // count, 0, 3 * (m % count)] // BPO for m in range(members)]
    ranks = []
    for m in range(members):
        rank = jnp.int32(0)
        for e in range(m):
            rank = rank + jnp.where(belongs[e] == belongs[m], 1, 0)
        ranks.append(rank)
    places = [belongs[m] * slots + ranks[m] for m in range(members)]

    chosen = []
    for slot in range(owners * slots):
        member = jnp.int32(0)
        for m in range(1, members):
            member = jnp.where(places[m] == slot, m, member)
        chosen.append(member)

    def forward(ahead, p, carry):
        drain(grouped.at[p, pl.ds(0, lanes - 1)], z_recv.at[p])
        if ahead is not None:
            send(p + ahead)

        staging[...] = grouped[p].reshape(members, rows, width)
        for slot, member in enumerate(chosen):
            outgoing[p, slot // slots, slot % slots] = staging[member]

        def ship(i, inner_carry):
            r_copy(p, i).start()
            return inner_carry

        lax.fori_loop(1, owners, ship, 0)
        got[p, row] = outgoing[p, row]
        return carry

    def arrival(p):
        return jnp.where(p < half, 1, jnp.where(p < CHUNKS - SPLIT, 2, 3))

    def r_copy(p, i):
        to = lax.rem(row + i, owners)
        return pltpu.make_async_remote_copy(
            src_ref=outgoing.at[p, to], dst_ref=got.at[p, row],
            send_sem=r_sems.at[0], recv_sem=r_sems.at[arrival(p)],
            device_id=at_row(to), device_id_type=MESH,
        )

    for k in range(2, 4):
        drain(all_v.at[pl.ds(0, owners - 1)], map_sems.at[k])
    all_scalar = pltpu.make_async_copy(all_v.at[:, :, pl.ds(0, 1)], all_s, small.at[7])
    all_scalar.start()
    all_scalar.wait()

    seats = owners * slots
    entries = len(PAIRS) * seats
    extent = entries + -entries % LANE
    limit = BPO * BAND

    def links():
        goals = [targets[c // seats, c % seats] for c in range(entries)]
        lane = lax.broadcasted_iota(jnp.int32, (8, extent), 1)
        sub = lax.broadcasted_iota(jnp.int32, (8, extent), 0)
        along = jnp.full((8, extent), -1, jnp.int32)
        for c in range(entries):
            along = jnp.where(lane == c, goals[c], along)
        before = jnp.full((8, extent), -1, jnp.int32)
        final = jnp.full((8, extent), -1, jnp.int32)
        for base in range(0, entries, 8):
            down = jnp.full((8, extent), -2, jnp.int32)
            for r in range(8):
                down = jnp.where(sub == r, goals[base + r], down)
            entry = sub + base
            before = jnp.where((down == along) & (entry < lane), entry, before)
            final = jnp.where(down == lane, entry, final)
        for kind, found in enumerate((before, final)):
            best = found[0:1]
            for r in range(1, 8):
                best = jnp.maximum(best, found[r : r + 1])
            links_v[kind : kind + 1] = jnp.where(best < 0, entries, best)
        to_links = pltpu.make_async_copy(links_v, links_s, small.at[6])
        to_links.start()
        to_links.wait()

    def chain(kind, p, carry):
        for seat in range(seats):
            c = p * seats + seat
            piece = got[pl.ds((kind * len(PAIRS) + p) * SPLIT, SPLIT), seat // slots, seat % slots]
            totals[kind, c] = piece.reshape(part, width) + totals[kind, links_s[0, c]]
        return carry

    def aim(group, carry):
        picked = [[jnp.int32(-1)] * 3 for _ in range(slots)]
        filled = jnp.int32(0)
        for m in range(members):
            at = [all_s[group, m // count, 0, 3 * (m % count) + k] for k in range(3)]
            mine = at[0] // BPO == row
            for slot in range(slots):
                hit = mine & (filled == slot)
                picked[slot] = [jnp.where(hit, at[k], picked[slot][k]) for k in range(3)]
            filled = filled + jnp.where(mine, 1, 0)
        for slot in range(slots):
            at = picked[slot]
            for p, (i, j) in enumerate(PAIRS):
                local = (at[i] - row * BPO) * BAND + at[j] - at[i]
                targets[p, group * slots + slot] = jnp.where(at[0] >= 0, local, BPO * BAND)
        return carry

    lax.fori_loop(0, owners, aim, 0)
    links()

    issued = LEAD
    steps = []
    for p in range(CHUNKS):
        wanted = min(p + 1 + (LEAD if p < half - LEAD else TURN if p < half - 1 else AHEAD), CHUNKS)
        steps.append(issued - p if wanted > issued else None)
        issued = max(issued, wanted if wanted <= issued + 1 else issued + 1)
    first = 0
    for p in range(1, CHUNKS + 1):
        if p == CHUNKS or steps[p] != steps[first]:
            lax.fori_loop(first, p, functools.partial(forward, steps[first]), 0)
            first = p

    def arrived(first, last, k):
        drain(got.at[pl.ds(first, last - first), pl.ds(0, owners - 1)], r_sems.at[k])

    def gather(kind, band, first, last):
        def row_block(g, carry):
            for d in range(first, last):
                band[g * BAND + d] = totals[kind, links_s[1, g * BAND + d]]
            return carry

        lax.fori_loop(0, BPO, row_block, 0)

    for kind in range(KINDS):
        totals[kind, entries] = jnp.zeros((part, width), jnp.float32)
    arrived(0, half, 1)
    lax.fori_loop(0, len(PAIRS), functools.partial(chain, 0), 0)
    gather(0, k_band, 0, BAND)
    arrived(half, CHUNKS - SPLIT, 2)
    lax.fori_loop(0, len(PAIRS) - 1, functools.partial(chain, 1), 0)
    gather(1, m_band, 0, 2)
    drain(grouped.at[:, pl.ds(0, lanes - 1)], z_send)
    arrived(CHUNKS - SPLIT, CHUNKS, 3)
    chain(1, len(PAIRS) - 1, 0)
    gather(1, m_band, 2, BAND)
    drain(got.at[:, pl.ds(0, owners - 1)], r_sems.at[0])


def hand_out(k_band, m_band, coupled, k_out, m_out, coupling, sems):
    writes = [
        pltpu.make_async_copy(source, out, sems.at[i])
        for i, (source, out) in enumerate(((k_band, k_out), (m_band, m_out), (coupled, coupling)))
    ]
    for write in writes:
        write.start()
    for write in writes:
        write.wait()


def per_device(
    stiff_bb, stiff_bi, constraint_modes, interior_mass, fixed_modes, mass_bb, boundary_map
):
    owners = lax.axis_size("row")
    lanes = lax.axis_size("col")
    count, order, inner = stiff_bi.shape
    modes = fixed_modes.shape[2]
    width = order // 3
    part = width // lanes
    rows = part // SPLIT
    slots = (count * lanes + owners - 1) // owners
    f32, bf16 = jnp.float32, jnp.bfloat16
    hbm = pl.BlockSpec(memory_space=pltpu.HBM)
    vmem = pl.BlockSpec(memory_space=pltpu.VMEM)
    dma = pltpu.SemaphoreType.DMA
    seats = owners * slots
    entries = len(PAIRS) * seats
    extent = entries + -entries % LANE
    band = pltpu.VMEM((BPO * BAND, part, width), f32)
    bands = pl.pallas_call(
        functools.partial(reduce_and_send, owners, lanes, slots),
        out_shape=(
            band,
            band,
            pltpu.VMEM((count, modes, order), f32),
        ),
        in_specs=[hbm] * 7,
        out_specs=(vmem, vmem, vmem),
        scratch_shapes=[
            pltpu.VMEM((CHUNKS, owners, slots, rows, width), f32),
            pltpu.VMEM((KINDS, entries + 1, part, width), f32),
            pltpu.SMEM((len(PAIRS), seats), jnp.int32),
            pltpu.VMEM((KINDS, extent), jnp.int32),
            pltpu.SMEM((KINDS, extent), jnp.int32),
            pltpu.VMEM((count, 3, width, order), bf16),
            pltpu.VMEM((count, order, inner), bf16),
            pltpu.VMEM((count, inner, order), bf16),
            pltpu.VMEM((count, inner, modes), bf16),
            pltpu.VMEM((count, 3, width, order), bf16),
            pltpu.VMEM((count, inner), f32),
            pltpu.VMEM((count, inner, order), bf16),
            pltpu.VMEM((CHUNKS, lanes, count, rows, width), f32),
            pltpu.VMEM((CHUNKS, lanes, count, rows, width), f32),
            pltpu.VMEM((lanes * count, rows, width), f32),
            pltpu.VMEM((CHUNKS, owners, slots, rows, width), f32),
            pltpu.VMEM((8, LANE), jnp.int32),
            pltpu.VMEM((lanes, 8, LANE), jnp.int32),
            pltpu.VMEM((owners, lanes, 8, LANE), jnp.int32),
            pltpu.SMEM((count, 3), jnp.int32),
            pltpu.SMEM((lanes, 8, LANE), jnp.int32),
            pltpu.SMEM((owners, lanes, 1, LANE), jnp.int32),
            dma((2, count)),
            dma,
            dma((CHUNKS,)),
            dma((4,)),
            dma((4,)),
            dma((8,)),
            dma((2, 3)),
        ],
        compiler_params=pltpu.CompilerParams(
            collective_id=0, has_side_effects=True, vmem_limit_bytes=VMEM_LIMIT
        ),
        name="reduce_and_send",
    )(*(
        pltpu.with_memory_space_constraint(x, pltpu.HBM)
        for x in (stiff_bb, stiff_bi, constraint_modes, interior_mass, fixed_modes, mass_bb, boundary_map)
    ))
    block = jax.ShapeDtypeStruct(band.shape, f32)
    k_out, m_out, coupling = pl.pallas_call(
        hand_out,
        out_shape=(block, block, jax.ShapeDtypeStruct((count, modes, order), f32)),
        in_specs=[vmem] * 3,
        out_specs=(hbm, hbm, hbm),
        scratch_shapes=[dma((3,))],
        compiler_params=pltpu.CompilerParams(vmem_limit_bytes=BAND_LIMIT),
        name="hand_out",
    )(*bands)
    shape = (BPO, BAND, part, width)
    return k_out.reshape(shape), m_out.reshape(shape), coupling


def solution(mesh):
    placed = (
        P(("row", "col"), None, None, None),
        P(("row", "col"), None, None),
        P(("row", "col"), None, None),
        P(("row", "col"), None),
        P(("row", "col"), None, None),
        P(("row", "col"), None, None, None),
        P(("row", "col"), None),
    )
    return jax.shard_map(
        per_device,
        mesh=mesh,
        in_specs=placed,
        out_specs=(
            P("row", None, "col", None),
            P("row", None, "col", None),
            P(("row", "col"), None, None),
        ),
        check_vma=False,
    )
```

```python
import functools
import jax
import jax.numpy as jnp
from jax import lax
from jax.experimental import pallas as pl
from jax.experimental.pallas import tpu as pltpu
from jax.sharding import PartitionSpec as P

BAND = 4
BPO = 24
LANE = 128

PAIRS = ((0, 0), (0, 1), (1, 1), (1, 2), (2, 2), (0, 2))
KINDS = 2
CHUNKS = KINDS * len(PAIRS)
LAST = CHUNKS - 1
STEPS = (4, 5, None, 6, None, 7, 8, 9, 10, 11, None, None)
LEAD = 4
MESH = pl.DeviceIdType.MESH
VMEM_LIMIT = 55 * 1024 * 1024
BAND_LIMIT = 1024 * 1024


def at_col(z):
    return {"row": lax.axis_index("row"), "col": z}


def at_row(r):
    return {"row": r, "col": lax.axis_index("col")}


def reduce_and_send(
    owners, lanes, slots,
    kbb, kbi, psi, mass, modes, mbb, table,
    k_band, m_band, coupled,
    got, totals, targets, links_v, links_s,
    kbb_v, kbi_v, psi_v, modes_v, mbb_v, mass_v, weighted,
    reduced, grouped, staging, outgoing, table_v, maps_v, all_v, table_s, maps_s, all_s,
    load_sems, z_send, z_recv, r_sems, map_sems, small, block_sems,
):
    count, order, inner = kbi.shape
    width = order // 3
    part = width // lanes
    members = count * lanes
    row = lax.axis_index("row")
    col = lax.axis_index("col")

    def block_load(i):
        span = pl.ds(i * width, width)
        return (
            pltpu.make_async_copy(kbi.at[0, span], kbi_v.at[0, span], block_sems.at[0, i]),
            pltpu.make_async_copy(psi.at[0, :, span], psi_v.at[0, :, span], block_sems.at[1, i]),
        )

    def loads(s):
        return (
            pltpu.make_async_copy(kbi.at[s], kbi_v.at[s], load_sems.at[0, s - 1]),
            pltpu.make_async_copy(psi.at[s], psi_v.at[s], load_sems.at[1, s - 1]),
        )

    first_kbb = pltpu.make_async_copy(kbb.at[0], kbb_v.at[0], small.at[0])
    others = pl.ds(1, count - 1)
    other_kbb = pltpu.make_async_copy(kbb.at[others], kbb_v.at[others], small.at[1])
    late_loads = (
        pltpu.make_async_copy(mass, mass_v, small.at[2]),
        pltpu.make_async_copy(mbb, mbb_v, small.at[3]),
        pltpu.make_async_copy(modes, modes_v, small.at[4]),
    )

    for copy in block_load(2):
        copy.start()
    first_kbb.start()
    table_load = pltpu.make_async_copy(table, table_s, small.at[5])
    table_load.start()

    barrier = pltpu.get_barrier_semaphore()
    for i in range(1, lanes):
        pl.semaphore_signal(barrier, inc=1, device_id=at_col(lax.rem(col + i, lanes)), device_id_type=MESH)

    def greet(i, carry):
        pl.semaphore_signal(barrier, inc=1, device_id=at_row(lax.rem(row + i, owners)), device_id_type=MESH)
        return carry

    lax.fori_loop(1, owners, greet, 0)

    def put(kind, s, i, strip):
        for j in range(i, 3):
            block = strip[:, (j - i) * width : (j - i + 1) * width]
            reduced[kind * len(PAIRS) + PAIRS.index((i, j)), :, s] = block.reshape(lanes, part, width)

    def stiff(s, i):
        strip = jnp.dot(
            kbi_v[s, i * width : (i + 1) * width, :], psi_v[s, :, i * width :],
            preferred_element_type=jnp.float32,
        )
        put(0, s, i, strip + kbb_v[s, i, :, i * width :].astype(jnp.float32))

    def drain(ref, sem):
        pltpu.make_async_copy(ref, ref, sem).wait()

    def z_map(i):
        return pltpu.make_async_remote_copy(
            src_ref=table_v, dst_ref=maps_v.at[col],
            send_sem=map_sems.at[0], recv_sem=map_sems.at[1],
            device_id=at_col(lax.rem(col + i, lanes)), device_id_type=MESH,
        )

    def z_copy(p, i):
        to = lax.rem(col + i, lanes)
        return pltpu.make_async_remote_copy(
            src_ref=reduced.at[p, to], dst_ref=grouped.at[p, col],
            send_sem=z_send, recv_sem=z_recv.at[p],
            device_id=at_col(to), device_id_type=MESH,
        )

    def z_copy_part(p, first, size, i):
        to = lax.rem(col + i, lanes)
        return pltpu.make_async_remote_copy(
            src_ref=reduced.at[p, to, pl.ds(first, size)], dst_ref=grouped.at[p, col, pl.ds(first, size)],
            send_sem=z_send, recv_sem=z_recv.at[p],
            device_id=at_col(to), device_id_type=MESH,
        )

    def r_map(i):
        return pltpu.make_async_remote_copy(
            src_ref=maps_v, dst_ref=all_v.at[row],
            send_sem=map_sems.at[2], recv_sem=map_sems.at[3],
            device_id=at_row(lax.rem(row + i, owners)), device_id_type=MESH,
        )

    half = CHUNKS // KINDS
    table_load.wait()
    for i in (1, 0):
        for copy in block_load(i):
            copy.start()
    place = (lax.broadcasted_iota(jnp.int32, (8, LANE), 0), lax.broadcasted_iota(jnp.int32, (8, LANE), 1))
    tile = jnp.zeros((8, LANE), jnp.int32)
    for s in range(count):
        for k in range(3):
            tile = jnp.where((place[0] == 0) & (place[1] == 3 * s + k), table_s[s, k], tile)
    table_v[...] = tile
    maps_v[col] = tile

    first_kbb.wait()
    for i in reversed(range(3)):
        for copy in block_load(i):
            copy.wait()
        if i == 1:
            for later in range(1, count):
                for copy in loads(later):
                    copy.start()
            other_kbb.start()
            for copy in late_loads:
                copy.start()
        stiff(0, i)
        if i == 2:
            pl.semaphore_wait(barrier, lanes - 1 + owners - 1)
            for k in range(1, lanes):
                z_map(k).start()
        for j in range(i, 3):
            for k in range(1, lanes):
                z_copy_part(PAIRS.index((i, j)), 0, 1, k).start()

    other_kbb.wait()

    def stiffs(s, carry):
        for copy in loads(s):
            copy.wait()
        for i in range(3):
            stiff(s, i)
        return carry

    lax.fori_loop(1, count, stiffs, 0)

    def send(p):
        @pl.when(p < half)
        def _():
            for k in range(1, lanes):
                z_copy_part(p, 1, count - 1, k).start()

        @pl.when(p >= half)
        def _():
            for k in range(1, lanes):
                z_copy(p, k).start()

    for p in range(LEAD):
        send(p)

    def masses(s, carry):
        pick = lax.broadcasted_iota(jnp.int32, (count, inner), 0) == s
        line = jnp.sum(jnp.where(pick, mass_v[...], 0.0), axis=0, keepdims=True)
        steps = inner // LANE
        lines = [line[:, k * LANE : (k + 1) * LANE] for k in range(steps)]
        filler = jnp.zeros((-steps % LANE, LANE), jnp.float32)
        columns = jnp.concatenate(lines + [filler], axis=0).T
        for k in range(steps):
            span = pl.ds(k * LANE, LANE)
            scale = jnp.broadcast_to(columns[:, k : k + 1], (LANE, order))
            weighted[s, span, :] = (scale * psi_v[s, span, :].astype(jnp.float32)).astype(jnp.bfloat16)
        for i in range(3):
            strip = lax.dot_general(
                psi_v[s, :, i * width : (i + 1) * width], weighted[s, :, i * width :], across,
                preferred_element_type=jnp.float32,
            )
            put(1, s, i, strip + mbb_v[s, i, :, i * width :].astype(jnp.float32))
        return carry

    across = (((0,), (0,)), ((), ()))
    for copy in late_loads:
        copy.wait()
    lax.fori_loop(0, count, masses, 0)

    for k in range(2):
        drain(maps_v.at[pl.ds(0, lanes - 1)], map_sems.at[k])
    to_scalar = pltpu.make_async_copy(maps_v, maps_s, small.at[5])
    to_scalar.start()
    lax.fori_loop(1, owners, lambda i, c: (r_map(i).start(), c)[1], 0)
    all_v[row] = maps_v[...]

    def couple(s, carry):
        coupled[s] = lax.dot_general(modes_v[s], weighted[s], across, preferred_element_type=jnp.float32)
        return carry

    def keep(p, carry):
        grouped[p, col] = reduced[p, col]
        return carry

    lax.fori_loop(0, CHUNKS, keep, 0)
    lax.fori_loop(0, count, couple, 0)

    to_scalar.wait()

    belongs = [maps_s[m // count, 0, 3 * (m % count)] // BPO for m in range(members)]
    ranks = []
    for m in range(members):
        rank = jnp.int32(0)
        for e in range(m):
            rank = rank + jnp.where(belongs[e] == belongs[m], 1, 0)
        ranks.append(rank)
    places = [belongs[m] * slots + ranks[m] for m in range(members)]

    chosen = []
    for slot in range(owners * slots):
        member = jnp.int32(0)
        for m in range(1, members):
            member = jnp.where(places[m] == slot, m, member)
        chosen.append(member)

    def forward(ahead, p, carry):
        drain(grouped.at[p, pl.ds(0, lanes - 1)], z_recv.at[p])
        if ahead is not None:
            send(p + ahead)

        staging[...] = grouped[p].reshape(members, part, width)
        for slot, member in enumerate(chosen):
            outgoing[p, slot // slots, slot % slots] = staging[member]

        def ship(i, inner_carry):
            r_copy(p, i).start()
            return inner_carry

        lax.fori_loop(1, owners, ship, 0)
        got[p, row] = outgoing[p, row]
        return carry

    def arrival(p):
        return jnp.where(p < half, 1, jnp.where(p < LAST, 2, 3))

    def r_copy(p, i):
        to = lax.rem(row + i, owners)
        return pltpu.make_async_remote_copy(
            src_ref=outgoing.at[p, to], dst_ref=got.at[p, row],
            send_sem=r_sems.at[0], recv_sem=r_sems.at[arrival(p)],
            device_id=at_row(to), device_id_type=MESH,
        )

    for k in range(2, 4):
        drain(all_v.at[pl.ds(0, owners - 1)], map_sems.at[k])
    all_scalar = pltpu.make_async_copy(all_v.at[:, :, pl.ds(0, 1)], all_s, small.at[5])
    all_scalar.start()
    all_scalar.wait()

    seats = owners * slots
    entries = len(PAIRS) * seats
    extent = entries + -entries % LANE
    limit = BPO * BAND

    def links():
        goals = [targets[c // seats, c % seats] for c in range(entries)]
        lane = lax.broadcasted_iota(jnp.int32, (8, extent), 1)
        sub = lax.broadcasted_iota(jnp.int32, (8, extent), 0)
        along = jnp.full((8, extent), -1, jnp.int32)
        for c in range(entries):
            along = jnp.where(lane == c, goals[c], along)
        before = jnp.full((8, extent), -1, jnp.int32)
        final = jnp.full((8, extent), -1, jnp.int32)
        for base in range(0, entries, 8):
            down = jnp.full((8, extent), -2, jnp.int32)
            for r in range(8):
                down = jnp.where(sub == r, goals[base + r], down)
            entry = sub + base
            before = jnp.where((down == along) & (entry < lane), entry, before)
            final = jnp.where(down == lane, entry, final)
        for kind, found in enumerate((before, final)):
            best = found[0:1]
            for r in range(1, 8):
                best = jnp.maximum(best, found[r : r + 1])
            links_v[kind : kind + 1] = jnp.where(best < 0, entries, best)
        to_links = pltpu.make_async_copy(links_v, links_s, small.at[5])
        to_links.start()
        to_links.wait()

    def chain(kind, p, carry):
        for seat in range(seats):
            c = p * seats + seat
            piece = got[kind * len(PAIRS) + p, seat // slots, seat % slots]
            totals[kind, c] = piece + totals[kind, links_s[0, c]]
        return carry

    def aim(group, carry):
        picked = [[jnp.int32(-1)] * 3 for _ in range(slots)]
        filled = jnp.int32(0)
        for m in range(members):
            at = [all_s[group, m // count, 0, 3 * (m % count) + k] for k in range(3)]
            mine = at[0] // BPO == row
            for slot in range(slots):
                hit = mine & (filled == slot)
                picked[slot] = [jnp.where(hit, at[k], picked[slot][k]) for k in range(3)]
            filled = filled + jnp.where(mine, 1, 0)
        for slot in range(slots):
            at = picked[slot]
            for p, (i, j) in enumerate(PAIRS):
                local = (at[i] - row * BPO) * BAND + at[j] - at[i]
                targets[p, group * slots + slot] = jnp.where(at[0] >= 0, local, BPO * BAND)
        return carry

    lax.fori_loop(0, owners, aim, 0)
    links()

    steps = [None if c is None else c - p for p, c in enumerate(STEPS)]
    first = 0
    for p in range(1, CHUNKS + 1):
        if p == CHUNKS or steps[p] != steps[first]:
            lax.fori_loop(first, p, functools.partial(forward, steps[first]), 0)
            first = p

    def arrived(first, last, k):
        drain(got.at[pl.ds(first, last - first), pl.ds(0, owners - 1)], r_sems.at[k])

    def gather(kind, band, first, last):
        def row_block(g, carry):
            for d in range(first, last):
                band[g * BAND + d] = totals[kind, links_s[1, g * BAND + d]]
            return carry

        lax.fori_loop(0, BPO, row_block, 0)

    for kind in range(KINDS):
        totals[kind, entries] = jnp.zeros((part, width), jnp.float32)
    arrived(0, half, 1)
    lax.fori_loop(0, len(PAIRS), functools.partial(chain, 0), 0)
    gather(0, k_band, 0, BAND)
    arrived(half, LAST, 2)
    lax.fori_loop(0, len(PAIRS) - 1, functools.partial(chain, 1), 0)
    gather(1, m_band, 0, 2)
    drain(grouped.at[:, pl.ds(0, lanes - 1)], z_send)
    arrived(LAST, CHUNKS, 3)
    chain(1, len(PAIRS) - 1, 0)
    gather(1, m_band, 2, BAND)
    drain(got.at[:, pl.ds(0, owners - 1)], r_sems.at[0])


def hand_out(k_band, m_band, coupled, k_out, m_out, coupling, sems):
    writes = [
        pltpu.make_async_copy(source, out, sems.at[i])
        for i, (source, out) in enumerate(((k_band, k_out), (m_band, m_out), (coupled, coupling)))
    ]
    for write in writes:
        write.start()
    for write in writes:
        write.wait()


def per_device(
    stiff_bb, stiff_bi, constraint_modes, interior_mass, fixed_modes, mass_bb, boundary_map
):
    owners = lax.axis_size("row")
    lanes = lax.axis_size("col")
    count, order, inner = stiff_bi.shape
    modes = fixed_modes.shape[2]
    width = order // 3
    part = width // lanes
    slots = (count * lanes + owners - 1) // owners
    f32, bf16 = jnp.float32, jnp.bfloat16
    hbm = pl.BlockSpec(memory_space=pltpu.HBM)
    vmem = pl.BlockSpec(memory_space=pltpu.VMEM)
    dma = pltpu.SemaphoreType.DMA
    seats = owners * slots
    entries = len(PAIRS) * seats
    extent = entries + -entries % LANE
    band = pltpu.VMEM((BPO * BAND, part, width), f32)
    bands = pl.pallas_call(
        functools.partial(reduce_and_send, owners, lanes, slots),
        out_shape=(
            band,
            band,
            pltpu.VMEM((count, modes, order), f32),
        ),
        in_specs=[hbm] * 7,
        out_specs=(vmem, vmem, vmem),
        scratch_shapes=[
            pltpu.VMEM((CHUNKS, owners, slots, part, width), f32),
            pltpu.VMEM((KINDS, entries + 1, part, width), f32),
            pltpu.SMEM((len(PAIRS), seats), jnp.int32),
            pltpu.VMEM((KINDS, extent), jnp.int32),
            pltpu.SMEM((KINDS, extent), jnp.int32),
            pltpu.VMEM((count, 3, width, order), bf16),
            pltpu.VMEM((count, order, inner), bf16),
            pltpu.VMEM((count, inner, order), bf16),
            pltpu.VMEM((count, inner, modes), bf16),
            pltpu.VMEM((count, 3, width, order), bf16),
            pltpu.VMEM((count, inner), f32),
            pltpu.VMEM((count, inner, order), bf16),
            pltpu.VMEM((CHUNKS, lanes, count, part, width), f32),
            pltpu.VMEM((CHUNKS, lanes, count, part, width), f32),
            pltpu.VMEM((lanes * count, part, width), f32),
            pltpu.VMEM((CHUNKS, owners, slots, part, width), f32),
            pltpu.VMEM((8, LANE), jnp.int32),
            pltpu.VMEM((lanes, 8, LANE), jnp.int32),
            pltpu.VMEM((owners, lanes, 8, LANE), jnp.int32),
            pltpu.SMEM((count, 3), jnp.int32),
            pltpu.SMEM((lanes, 8, LANE), jnp.int32),
            pltpu.SMEM((owners, lanes, 1, LANE), jnp.int32),
            dma((2, count - 1)),
            dma,
            dma((CHUNKS,)),
            dma((4,)),
            dma((4,)),
            dma((6,)),
            dma((2, 3)),
        ],
        compiler_params=pltpu.CompilerParams(
            collective_id=0, has_side_effects=True, vmem_limit_bytes=VMEM_LIMIT
        ),
        name="reduce_and_send",
    )(*(
        pltpu.with_memory_space_constraint(x, pltpu.HBM)
        for x in (stiff_bb, stiff_bi, constraint_modes, interior_mass, fixed_modes, mass_bb, boundary_map)
    ))
    block = jax.ShapeDtypeStruct(band.shape, f32)
    k_out, m_out, coupling = pl.pallas_call(
        hand_out,
        out_shape=(block, block, jax.ShapeDtypeStruct((count, modes, order), f32)),
        in_specs=[vmem] * 3,
        out_specs=(hbm, hbm, hbm),
        scratch_shapes=[dma((3,))],
        compiler_params=pltpu.CompilerParams(vmem_limit_bytes=BAND_LIMIT),
        name="hand_out",
    )(*bands)
    shape = (BPO, BAND, part, width)
    return k_out.reshape(shape), m_out.reshape(shape), coupling


def solution(mesh):
    placed = (
        P(("row", "col"), None, None, None),
        P(("row", "col"), None, None),
        P(("row", "col"), None, None),
        P(("row", "col"), None),
        P(("row", "col"), None, None),
        P(("row", "col"), None, None, None),
        P(("row", "col"), None),
    )
    return jax.shard_map(
        per_device,
        mesh=mesh,
        in_specs=placed,
        out_specs=(
            P("row", None, "col", None),
            P("row", None, "col", None),
            P(("row", "col"), None, None),
        ),
        check_vma=False,
    )
```

```python
import functools
import jax
import jax.numpy as jnp
from jax import lax
from jax.experimental import pallas as pl
from jax.experimental.pallas import tpu as pltpu
from jax.sharding import PartitionSpec as P

BAND = 4
BPO = 24
LANE = 128

PAIRS = ((0, 0), (0, 1), (1, 1), (1, 2), (2, 2), (0, 2))
KINDS = 2
CHUNKS = KINDS * len(PAIRS)
LAST = CHUNKS - 1
STEPS = (4, 5, None, 6, None, 7, 8, 9, 10, 11, None, None)
LEAD = 4
MESH = pl.DeviceIdType.MESH
VMEM_LIMIT = 55 * 1024 * 1024
BAND_LIMIT = 1024 * 1024


def at_col(z):
    return {"row": lax.axis_index("row"), "col": z}


def at_row(r):
    return {"row": r, "col": lax.axis_index("col")}


def reduce_and_send(
    owners, lanes, slots,
    kbb, kbi, psi, mass, modes, mbb, table,
    k_band, m_band, coupled,
    got, totals, targets, links_v, links_s,
    kbb_v, kbi_v, psi_v, modes_v, mbb_v, mass_v, weighted,
    reduced, grouped, staging, outgoing, table_v, maps_v, all_v, table_s, maps_s, all_s,
    load_sems, z_send, z_recv, r_sems, map_sems, small, block_sems,
):
    count, order, inner = kbi.shape
    width = order // 3
    part = width // lanes
    members = count * lanes
    row = lax.axis_index("row")
    col = lax.axis_index("col")

    def block_load(i):
        span = pl.ds(i * width, width)
        return (
            pltpu.make_async_copy(kbi.at[0, span], kbi_v.at[0, span], block_sems.at[0, i]),
            pltpu.make_async_copy(psi.at[0, :, span], psi_v.at[0, :, span], block_sems.at[1, i]),
        )

    def loads(s):
        return (
            pltpu.make_async_copy(kbi.at[s], kbi_v.at[s], load_sems.at[0, s - 1]),
            pltpu.make_async_copy(psi.at[s], psi_v.at[s], load_sems.at[1, s - 1]),
        )

    first_kbb = pltpu.make_async_copy(kbb.at[0], kbb_v.at[0], small.at[0])
    others = pl.ds(1, count - 1)
    other_kbb = pltpu.make_async_copy(kbb.at[others], kbb_v.at[others], small.at[1])
    late_loads = (
        pltpu.make_async_copy(mass, mass_v, small.at[2]),
        pltpu.make_async_copy(mbb, mbb_v, small.at[3]),
        pltpu.make_async_copy(modes, modes_v, small.at[4]),
    )

    for copy in block_load(2):
        copy.start()
    first_kbb.start()
    table_load = pltpu.make_async_copy(table, table_s, small.at[5])
    table_load.start()

    barrier = pltpu.get_barrier_semaphore()
    for i in range(1, lanes):
        pl.semaphore_signal(barrier, inc=1, device_id=at_col(lax.rem(col + i, lanes)), device_id_type=MESH)

    def greet(i, carry):
        pl.semaphore_signal(barrier, inc=1, device_id=at_row(lax.rem(row + i, owners)), device_id_type=MESH)
        return carry

    lax.fori_loop(1, owners, greet, 0)

    def put(kind, s, i, strip):
        for j in range(i, 3):
            block = strip[:, (j - i) * width : (j - i + 1) * width]
            reduced[kind * len(PAIRS) + PAIRS.index((i, j)), :, s] = block.reshape(lanes, part, width)

    def stiff(s, i):
        strip = jnp.dot(
            kbi_v[s, i * width : (i + 1) * width, :], psi_v[s, :, i * width :],
            preferred_element_type=jnp.float32,
        )
        put(0, s, i, strip + kbb_v[s, i, :, i * width :].astype(jnp.float32))

    def drain(ref, sem):
        pltpu.make_async_copy(ref, ref, sem).wait()

    def z_map(i):
        return pltpu.make_async_remote_copy(
            src_ref=table_v, dst_ref=maps_v.at[col],
            send_sem=map_sems.at[0], recv_sem=map_sems.at[1],
            device_id=at_col(lax.rem(col + i, lanes)), device_id_type=MESH,
        )

    def z_copy(p, i):
        to = lax.rem(col + i, lanes)
        return pltpu.make_async_remote_copy(
            src_ref=reduced.at[p, to], dst_ref=grouped.at[p, col],
            send_sem=z_send, recv_sem=z_recv.at[p],
            device_id=at_col(to), device_id_type=MESH,
        )

    def z_copy_part(p, first, size, i):
        to = lax.rem(col + i, lanes)
        return pltpu.make_async_remote_copy(
            src_ref=reduced.at[p, to, pl.ds(first, size)], dst_ref=grouped.at[p, col, pl.ds(first, size)],
            send_sem=z_send, recv_sem=z_recv.at[p],
            device_id=at_col(to), device_id_type=MESH,
        )

    def mirrored(i):
        to, bit = 0, 1
        while bit < owners:
            to = to + lax.rem(row // bit + i // bit, 2) * bit
            bit *= 2
        return to

    far_first = sorted(range(1, owners), key=lambda i: (-bin(i // 2).count("1"), -(i // 2), i))
    paired = owners & (owners - 1) == 0
    partners = [mirrored(i) if paired else lax.rem(row + i, owners) for i in far_first]

    def r_map(i):
        return pltpu.make_async_remote_copy(
            src_ref=maps_v, dst_ref=all_v.at[row],
            send_sem=map_sems.at[2], recv_sem=map_sems.at[3],
            device_id=at_row(lax.rem(row + i, owners)), device_id_type=MESH,
        )

    half = CHUNKS // KINDS
    table_load.wait()
    for i in (1, 0):
        for copy in block_load(i):
            copy.start()
    place = (lax.broadcasted_iota(jnp.int32, (8, LANE), 0), lax.broadcasted_iota(jnp.int32, (8, LANE), 1))
    tile = jnp.zeros((8, LANE), jnp.int32)
    for s in range(count):
        for k in range(3):
            tile = jnp.where((place[0] == 0) & (place[1] == 3 * s + k), table_s[s, k], tile)
    table_v[...] = tile
    maps_v[col] = tile

    first_kbb.wait()
    for i in reversed(range(3)):
        for copy in block_load(i):
            copy.wait()
        if i == 1:
            for later in range(1, count):
                for copy in loads(later):
                    copy.start()
            other_kbb.start()
            for copy in late_loads:
                copy.start()
        stiff(0, i)
        if i == 2:
            pl.semaphore_wait(barrier, lanes - 1 + owners - 1)
            for k in range(1, lanes):
                z_map(k).start()
        for j in range(i, 3):
            for k in range(1, lanes):
                z_copy_part(PAIRS.index((i, j)), 0, 1, k).start()

    other_kbb.wait()

    def stiffs(s, carry):
        for copy in loads(s):
            copy.wait()
        for i in range(3):
            stiff(s, i)
        return carry

    lax.fori_loop(1, count, stiffs, 0)

    def send(p):
        @pl.when(p < half)
        def _():
            for k in range(1, lanes):
                z_copy_part(p, 1, count - 1, k).start()

        @pl.when(p >= half)
        def _():
            for k in range(1, lanes):
                z_copy(p, k).start()

    for p in range(LEAD):
        send(p)

    def masses(s, carry):
        pick = lax.broadcasted_iota(jnp.int32, (count, inner), 0) == s
        line = jnp.sum(jnp.where(pick, mass_v[...], 0.0), axis=0, keepdims=True)
        steps = inner // LANE
        lines = [line[:, k * LANE : (k + 1) * LANE] for k in range(steps)]
        filler = jnp.zeros((-steps % LANE, LANE), jnp.float32)
        columns = jnp.concatenate(lines + [filler], axis=0).T
        for k in range(steps):
            span = pl.ds(k * LANE, LANE)
            scale = jnp.broadcast_to(columns[:, k : k + 1], (LANE, order))
            weighted[s, span, :] = (scale * psi_v[s, span, :].astype(jnp.float32)).astype(jnp.bfloat16)
        for i in range(3):
            strip = lax.dot_general(
                psi_v[s, :, i * width : (i + 1) * width], weighted[s, :, i * width :], across,
                preferred_element_type=jnp.float32,
            )
            put(1, s, i, strip + mbb_v[s, i, :, i * width :].astype(jnp.float32))
        return carry

    across = (((0,), (0,)), ((), ()))
    for copy in late_loads:
        copy.wait()
    lax.fori_loop(0, count, masses, 0)

    for k in range(2):
        drain(maps_v.at[pl.ds(0, lanes - 1)], map_sems.at[k])
    to_scalar = pltpu.make_async_copy(maps_v, maps_s, small.at[5])
    to_scalar.start()
    lax.fori_loop(1, owners, lambda i, c: (r_map(i).start(), c)[1], 0)
    all_v[row] = maps_v[...]

    def couple(s, carry):
        coupled[s] = lax.dot_general(modes_v[s], weighted[s], across, preferred_element_type=jnp.float32)
        return carry

    def keep(p, carry):
        grouped[p, col] = reduced[p, col]
        return carry

    lax.fori_loop(0, CHUNKS, keep, 0)
    lax.fori_loop(0, count, couple, 0)

    to_scalar.wait()

    belongs = [maps_s[m // count, 0, 3 * (m % count)] // BPO for m in range(members)]
    ranks = []
    for m in range(members):
        rank = jnp.int32(0)
        for e in range(m):
            rank = rank + jnp.where(belongs[e] == belongs[m], 1, 0)
        ranks.append(rank)
    places = [belongs[m] * slots + ranks[m] for m in range(members)]

    chosen = []
    for slot in range(owners * slots):
        member = jnp.int32(0)
        for m in range(1, members):
            member = jnp.where(places[m] == slot, m, member)
        chosen.append(member)

    def forward(ahead, p, carry):
        drain(grouped.at[p, pl.ds(0, lanes - 1)], z_recv.at[p])
        if ahead is not None:
            send(p + ahead)

        staging[...] = grouped[p].reshape(members, part, width)
        for slot, member in enumerate(chosen):
            outgoing[p, slot // slots, slot % slots] = staging[member]

        for to in partners:
            r_copy(p, to).start()
        got[p, row] = outgoing[p, row]
        return carry

    def arrival(p):
        return jnp.where(p < half, 1, jnp.where(p < LAST, 2, 3))

    def r_copy(p, to):
        return pltpu.make_async_remote_copy(
            src_ref=outgoing.at[p, to], dst_ref=got.at[p, row],
            send_sem=r_sems.at[0], recv_sem=r_sems.at[arrival(p)],
            device_id=at_row(to), device_id_type=MESH,
        )

    for k in range(2, 4):
        drain(all_v.at[pl.ds(0, owners - 1)], map_sems.at[k])
    all_scalar = pltpu.make_async_copy(all_v.at[:, :, pl.ds(0, 1)], all_s, small.at[5])
    all_scalar.start()
    all_scalar.wait()

    seats = owners * slots
    entries = len(PAIRS) * seats
    extent = entries + -entries % LANE
    limit = BPO * BAND

    def links():
        goals = [targets[c // seats, c % seats] for c in range(entries)]
        lane = lax.broadcasted_iota(jnp.int32, (8, extent), 1)
        sub = lax.broadcasted_iota(jnp.int32, (8, extent), 0)
        along = jnp.full((8, extent), -1, jnp.int32)
        for c in range(entries):
            along = jnp.where(lane == c, goals[c], along)
        before = jnp.full((8, extent), -1, jnp.int32)
        final = jnp.full((8, extent), -1, jnp.int32)
        for base in range(0, entries, 8):
            down = jnp.full((8, extent), -2, jnp.int32)
            for r in range(8):
                down = jnp.where(sub == r, goals[base + r], down)
            entry = sub + base
            before = jnp.where((down == along) & (entry < lane), entry, before)
            final = jnp.where(down == lane, entry, final)
        for kind, found in enumerate((before, final)):
            best = found[0:1]
            for r in range(1, 8):
                best = jnp.maximum(best, found[r : r + 1])
            links_v[kind : kind + 1] = jnp.where(best < 0, entries, best)
        to_links = pltpu.make_async_copy(links_v, links_s, small.at[5])
        to_links.start()
        to_links.wait()

    def chain(kind, p, carry):
        for seat in range(seats):
            c = p * seats + seat
            piece = got[kind * len(PAIRS) + p, seat // slots, seat % slots]
            totals[kind, c] = piece + totals[kind, links_s[0, c]]
        return carry

    def aim(group, carry):
        picked = [[jnp.int32(-1)] * 3 for _ in range(slots)]
        filled = jnp.int32(0)
        for m in range(members):
            at = [all_s[group, m // count, 0, 3 * (m % count) + k] for k in range(3)]
            mine = at[0] // BPO == row
            for slot in range(slots):
                hit = mine & (filled == slot)
                picked[slot] = [jnp.where(hit, at[k], picked[slot][k]) for k in range(3)]
            filled = filled + jnp.where(mine, 1, 0)
        for slot in range(slots):
            at = picked[slot]
            for p, (i, j) in enumerate(PAIRS):
                local = (at[i] - row * BPO) * BAND + at[j] - at[i]
                targets[p, group * slots + slot] = jnp.where(at[0] >= 0, local, BPO * BAND)
        return carry

    lax.fori_loop(0, owners, aim, 0)
    links()

    steps = [None if c is None else c - p for p, c in enumerate(STEPS)]
    first = 0
    for p in range(1, CHUNKS + 1):
        if p == CHUNKS or steps[p] != steps[first]:
            lax.fori_loop(first, p, functools.partial(forward, steps[first]), 0)
            first = p

    def arrived(first, last, k):
        drain(got.at[pl.ds(first, last - first), pl.ds(0, owners - 1)], r_sems.at[k])

    def gather(kind, band, first, last):
        def row_block(g, carry):
            for d in range(first, last):
                band[g * BAND + d] = totals[kind, links_s[1, g * BAND + d]]
            return carry

        lax.fori_loop(0, BPO, row_block, 0)

    for kind in range(KINDS):
        totals[kind, entries] = jnp.zeros((part, width), jnp.float32)
    arrived(0, half, 1)
    lax.fori_loop(0, len(PAIRS), functools.partial(chain, 0), 0)
    gather(0, k_band, 0, BAND)
    arrived(half, LAST, 2)
    lax.fori_loop(0, len(PAIRS) - 1, functools.partial(chain, 1), 0)
    gather(1, m_band, 0, 2)
    drain(grouped.at[:, pl.ds(0, lanes - 1)], z_send)
    arrived(LAST, CHUNKS, 3)
    chain(1, len(PAIRS) - 1, 0)
    gather(1, m_band, 2, BAND)
    drain(got.at[:, pl.ds(0, owners - 1)], r_sems.at[0])


def hand_out(k_band, m_band, coupled, k_out, m_out, coupling, sems):
    writes = [
        pltpu.make_async_copy(source, out, sems.at[i])
        for i, (source, out) in enumerate(((k_band, k_out), (m_band, m_out), (coupled, coupling)))
    ]
    for write in writes:
        write.start()
    for write in writes:
        write.wait()


def per_device(
    stiff_bb, stiff_bi, constraint_modes, interior_mass, fixed_modes, mass_bb, boundary_map
):
    owners = lax.axis_size("row")
    lanes = lax.axis_size("col")
    count, order, inner = stiff_bi.shape
    modes = fixed_modes.shape[2]
    width = order // 3
    part = width // lanes
    slots = (count * lanes + owners - 1) // owners
    f32, bf16 = jnp.float32, jnp.bfloat16
    hbm = pl.BlockSpec(memory_space=pltpu.HBM)
    vmem = pl.BlockSpec(memory_space=pltpu.VMEM)
    dma = pltpu.SemaphoreType.DMA
    seats = owners * slots
    entries = len(PAIRS) * seats
    extent = entries + -entries % LANE
    band = pltpu.VMEM((BPO * BAND, part, width), f32)
    bands = pl.pallas_call(
        functools.partial(reduce_and_send, owners, lanes, slots),
        out_shape=(
            band,
            band,
            pltpu.VMEM((count, modes, order), f32),
        ),
        in_specs=[hbm] * 7,
        out_specs=(vmem, vmem, vmem),
        scratch_shapes=[
            pltpu.VMEM((CHUNKS, owners, slots, part, width), f32),
            pltpu.VMEM((KINDS, entries + 1, part, width), f32),
            pltpu.SMEM((len(PAIRS), seats), jnp.int32),
            pltpu.VMEM((KINDS, extent), jnp.int32),
            pltpu.SMEM((KINDS, extent), jnp.int32),
            pltpu.VMEM((count, 3, width, order), bf16),
            pltpu.VMEM((count, order, inner), bf16),
            pltpu.VMEM((count, inner, order), bf16),
            pltpu.VMEM((count, inner, modes), bf16),
            pltpu.VMEM((count, 3, width, order), bf16),
            pltpu.VMEM((count, inner), f32),
            pltpu.VMEM((count, inner, order), bf16),
            pltpu.VMEM((CHUNKS, lanes, count, part, width), f32),
            pltpu.VMEM((CHUNKS, lanes, count, part, width), f32),
            pltpu.VMEM((lanes * count, part, width), f32),
            pltpu.VMEM((CHUNKS, owners, slots, part, width), f32),
            pltpu.VMEM((8, LANE), jnp.int32),
            pltpu.VMEM((lanes, 8, LANE), jnp.int32),
            pltpu.VMEM((owners, lanes, 8, LANE), jnp.int32),
            pltpu.SMEM((count, 3), jnp.int32),
            pltpu.SMEM((lanes, 8, LANE), jnp.int32),
            pltpu.SMEM((owners, lanes, 1, LANE), jnp.int32),
            dma((2, count - 1)),
            dma,
            dma((CHUNKS,)),
            dma((4,)),
            dma((4,)),
            dma((6,)),
            dma((2, 3)),
        ],
        compiler_params=pltpu.CompilerParams(
            collective_id=0, has_side_effects=True, vmem_limit_bytes=VMEM_LIMIT
        ),
        name="reduce_and_send",
    )(*(
        pltpu.with_memory_space_constraint(x, pltpu.HBM)
        for x in (stiff_bb, stiff_bi, constraint_modes, interior_mass, fixed_modes, mass_bb, boundary_map)
    ))
    block = jax.ShapeDtypeStruct(band.shape, f32)
    k_out, m_out, coupling = pl.pallas_call(
        hand_out,
        out_shape=(block, block, jax.ShapeDtypeStruct((count, modes, order), f32)),
        in_specs=[vmem] * 3,
        out_specs=(hbm, hbm, hbm),
        scratch_shapes=[dma((3,))],
        compiler_params=pltpu.CompilerParams(vmem_limit_bytes=BAND_LIMIT),
        name="hand_out",
    )(*bands)
    shape = (BPO, BAND, part, width)
    return k_out.reshape(shape), m_out.reshape(shape), coupling


def solution(mesh):
    placed = (
        P(("row", "col"), None, None, None),
        P(("row", "col"), None, None),
        P(("row", "col"), None, None),
        P(("row", "col"), None),
        P(("row", "col"), None, None),
        P(("row", "col"), None, None, None),
        P(("row", "col"), None),
    )
    return jax.shard_map(
        per_device,
        mesh=mesh,
        in_specs=placed,
        out_specs=(
            P("row", None, "col", None),
            P("row", None, "col", None),
            P(("row", "col"), None, None),
        ),
        check_vma=False,
    )
```
